256 devices in a mesh: shot: 8 (over y, core), tile: 32 (over x, z).
Axes of the slice: x: 4, y: 4, z: 8, core: 2. Of those that a mesh axis runs over, the one named last changes fastest.
Arguments:
- source: bfloat16 [512, 1, 128, 32, 128], P(('shot', 'tile')), may hold values from -6 to 6
- receiver: bfloat16 [512, 1, 128, 32, 128], P(('shot', 'tile')), may hold values from -6 to 6
- corners: int32 [512, 2], P(('shot', 'tile')), may hold values from 0 to 224, as said below
Outputs:
- filtered: float32 [128, 256, 256], P('tile', 'shot')
The draws below stay inside these ranges and needn't reach their ends.
Inputs may be any that keep to these rules, and one draw needn't show every extreme that they name: corners[s, 0] is at most 224 and corners[s, 1] at most 128, so every box lies inside the image.
All inputs are finite; a program needn't handle non-finite values.
Results may differ from the reference program's by a relative error of at most 0.0003.
Values may be sent and summed in bfloat16 or wider, within the bound.
A program may use at most 64 MiB of HBM per device.

```python
import jax
import jax.numpy as jnp
from jax import lax

NT = 1
X = 256
Y = 256
BX = 32
BY = 128
SHOTS = 512
Z = 128


def draw_corners(key, part):
    first_key, second_key = jax.random.split(jax.random.fold_in(key, 17))
    row_start = jax.random.randint(first_key, (SHOTS, 1), 0, X - BX + 1)
    col_start = jax.random.randint(second_key, (SHOTS, 1), 0, Y - BY + 1)
    return jnp.concatenate((row_start, col_start), axis=1).astype(jnp.int32)


def level_of(stream_key, dims, cuts, least, largest):
    factor_of = 1.0
    for axis_at, shards_of in cuts:
        steps = jax.random.uniform(jax.random.fold_in(jax.random.fold_in(stream_key, 6), axis_at), (shards_of,), jnp.float32, least / len(cuts), largest / len(cuts))
        factor_of = factor_of * jnp.repeat(jnp.exp(steps), dims[axis_at] // shards_of).reshape((-1,) + (1,) * (len(dims) - 1 - axis_at))
    return factor_of


def bell_draw(key, dims, spread, reach, cuts=(), kind=jnp.bfloat16):
    result = jax.random.normal(key, dims, jnp.float32) * spread
    if len(cuts) > 0:
        result = level_of(key, dims, cuts, -0.22, 0.18) * result
    return jnp.clip(result, min=-reach, max=reach).astype(kind)


def setup_inputs(seed: int = 0) -> dict:
    keys = jax.random.split(jax.random.key(seed), 4)
    return {
        "source": bell_draw(keys[0], (SHOTS, NT, Z, BX, BY), 1.0, 6.0, ((0, 256),)),
        "receiver": bell_draw(keys[1], (SHOTS, NT, Z, BX, BY), 1.0, 6.0, ((0, 256),)),
        "corners": draw_corners(jax.random.fold_in(keys[3], 71), 0),
    }


damping = 1.0


def reference(source, receiver, corners):
    def place(shot, totals):
        image, lights = totals
        wave = lax.dynamic_index_in_dim(source, shot, 0, keepdims=False).astype(jnp.float32)
        back = lax.dynamic_index_in_dim(receiver, shot, 0, keepdims=False).astype(jnp.float32)
        partial_value = jnp.sum(wave * back, axis=0)
        light = jnp.sum(wave * wave, axis=0)
        start = (jnp.int32(0), corners[shot, 0].astype(jnp.int32), corners[shot, 1].astype(jnp.int32))
        image = lax.dynamic_update_slice(image, lax.dynamic_slice(image, start, (Z, BX, BY)) + partial_value, start)
        lights = lax.dynamic_update_slice(lights, lax.dynamic_slice(lights, start, (Z, BX, BY)) + light, start)
        return image, lights

    empty = jnp.zeros((Z, X, Y), jnp.float32)
    image, lights = lax.fori_loop(0, SHOTS, place, (empty, empty))
    normal = image / (damping + lights)
    padded = jnp.pad(normal, 1)
    beside = padded[2:, 1:-1, 1:-1] + padded[:-2, 1:-1, 1:-1]
    beside = beside + padded[1:-1, 2:, 1:-1] + padded[1:-1, :-2, 1:-1]
    beside = beside + padded[1:-1, 1:-1, 2:] + padded[1:-1, 1:-1, :-2]
    return beside - 6.0 * normal
```

```python
import functools

import jax
import jax.numpy as jnp
from jax import lax
from jax.experimental import pallas as pl
from jax.experimental.pallas import tpu as pltpu
from jax.sharding import PartitionSpec as P

MESH = pl.DeviceIdType.MESH
NX, NY, NZ, NC = 4, 4, 8, 2
GROUP = NX * NY * NC
PLANES = NY
X = 256
Y = 256
BX = 32
BY = 128
STRIP = 32
F32 = jnp.float32
BF16 = jnp.bfloat16

ORDER = (
    (1, 0), (0, 1), (3, 3), (2, 1), (0, 3), (1, 2), (3, 0), (2, 2),
    (1, 1), (0, 2), (3, 1), (2, 3), (1, 3), (3, 2), (2, 0), (0, 0),
)


def kernel(
    corners_ref, src_hbm, rcv_hbm, out_ref,
    lbuf, sbuf, rbuf, cmsg, cland, rows, mask, obuf, cbuf, nbuf, fbuf,
    lsem, asend, arecv, csend, crecv, bsend, brecv, nsend, hsend, frecv,
):
    me_w = lax.axis_index("shot")
    me_t = lax.axis_index("tile")
    y, c = me_w // NC, lax.rem(me_w, NC)
    x, z = me_t // NZ, lax.rem(me_t, NZ)
    me_g = x * (NY * NC) + me_w
    up, down = lax.rem(z + 1, NZ), lax.rem(z + NZ - 1, NZ)

    def chip(dx, dy):
        return lax.rem(x + dx, NX), lax.rem(y + dy, NY)

    def remote(src, dst, send, recv, w, t):
        return pltpu.make_async_remote_copy(
            src_ref=src, dst_ref=dst, send_sem=send, recv_sem=recv,
            device_id=(w, t), device_id_type=MESH,
        )

    def depth_of(k):
        half = k // 2
        step = jnp.where(lax.rem(k, 2) == 0, half + 4, 3 - half)
        return lax.rem(z + step, NZ)

    def load(k):
        zt = depth_of(k)
        return (
            pltpu.make_async_copy(src_hbm.at[:, :, zt], lbuf.at[k, 0], lsem.at[k, 0]),
            pltpu.make_async_copy(rcv_hbm.at[:, :, zt], lbuf.at[k, 1], lsem.at[k, 1]),
        )

    @pl.loop(0, NZ)
    def _(k):
        for copy in load(k):
            copy.start()

    barrier = pltpu.get_barrier_semaphore()

    def greet(w, t):
        pl.semaphore_signal(barrier, inc=1, device_id=(w, t), device_id_type=MESH)

    @pl.loop(1, GROUP)
    def _(g):
        other = lax.rem(me_g + g, GROUP)
        greet(lax.rem(other, NY * NC), (other // (NY * NC)) * NZ + z)

    for k in range(NC):
        greet(y * NC + k, x * NZ + up)
        greet(y * NC + k, x * NZ + down)
    last = NX * NZ - 1

    @pl.loop(0, NY * NC)
    def _(w):
        @pl.when(me_t > 0)
        def _():
            greet(w, me_t - 1)

        @pl.when(me_t < last)
        def _():
            greet(w, me_t + 1)

    first_col = [corners_ref[k, 1] for k in range(2)]
    lane = lax.broadcasted_iota(jnp.int32, (1, 128), 1)
    a = lax.rem(lane, BX)
    cmsg[...] = jnp.where(
        lane < 32,
        corners_ref[0, 0] + a,
        jnp.where(
            lane < 64,
            corners_ref[1, 0] + a,
            jnp.where(lane < 96, first_col[0] + 0 * lane, first_col[1] + 0 * lane),
        ),
    )
    cland[me_g] = cmsg[...]
    edges = (me_t > 0).astype(jnp.int32) + (me_t < last).astype(jnp.int32)
    pl.semaphore_wait(barrier, GROUP - 1 + 2 * NC + NY * NC * edges)

    @pl.loop(1, GROUP)
    def _(g):
        other = lax.rem(me_g + g, GROUP)
        remote(
            cmsg, cland.at[me_g], csend, crecv,
            lax.rem(other, NY * NC), (other // (NY * NC)) * NZ + z,
        ).start()

    @pl.loop(0, NZ)
    def _(k):
        for copy in load(k):
            copy.wait()
        for which in range(2):
            for shot in range(2):
                block = lbuf[k, which, shot].reshape(NX * NY * BX, BY).astype(F32)
                block = pltpu.roll(block, lax.rem(first_col[shot], BY), 1).astype(BF16)
                sbuf[pl.ds(k * 16, 16), which, shot] = block.reshape(NX * NY, BX, BY)
        core, q = lax.rem(k, 2), k // 2
        for dx, dy in ORDER:
            tx, ty = chip(dx, dy)

            def send():
                remote(
                    sbuf.at[k * 16 + tx * NY + ty], rbuf.at[q, me_g], asend, arecv.at[q],
                    ty * NC + core, tx * NZ + z,
                ).start()

            if (dx, dy) == (0, 0):
                pl.when(core != c)(send)
            else:
                send()

        @pl.when(core == c)
        def _():
            rbuf[q, me_g] = sbuf[k * 16 + x * NY + y]

    pltpu.make_async_copy(cland.at[pl.ds(0, GROUP - 1)], cland.at[pl.ds(0, GROUP - 1)], crecv).wait()

    @pl.loop(0, GROUP // 4)
    def _(i):
        row = lax.broadcasted_iota(jnp.int32, (X, 128), 0)
        for h in range(2):
            one = cland[4 * i + 2 * h]
            two = cland[4 * i + 2 * h + 1]
            both = jnp.where(lane < 64, one, pltpu.roll(two, 64, 1))
            rows[i, :, pl.ds(h * 128, 128)] = (row == both).astype(F32).astype(BF16)
        wide = lax.broadcasted_iota(jnp.int32, (BX, 128), 1)
        for s in range(4):
            msg = cland[4 * i + s]
            for shot in range(2):
                col = msg[:, 64 + 32 * shot : 65 + 32 * shot]
                left = (wide >= col).astype(F32).astype(BF16)
                mask[i, pl.ds((2 * s + shot) * BX, BX), :] = left

    def place(q):
        pltpu.make_async_copy(
            rbuf.at[q, pl.ds(0, GROUP - 1)], rbuf.at[q, pl.ds(0, GROUP - 1)], arecv.at[q]
        ).wait()

        def step(i, fresh):
            got = rbuf[q, pl.ds(4 * i, 4)]
            wave = got[:, 0].reshape(256, BY).astype(F32)
            back = got[:, 1].reshape(256, BY).astype(F32)
            keep = mask[i]
            table = rows[i]
            for which, value in ((0, wave * back), (1, wave * wave)):
                hi = value.astype(BF16)
                lo = (value - hi.astype(F32)).astype(BF16)
                hi_left, lo_left = hi * keep, lo * keep
                hi_both = jnp.concatenate((hi_left, hi - hi_left), axis=1)
                lo_both = jnp.concatenate((lo_left, lo - lo_left), axis=1)
                part = jnp.dot(table, hi_both, preferred_element_type=F32)
                part = part + jnp.dot(table, lo_both, preferred_element_type=F32)
                if fresh:
                    obuf[q, which] = part
                else:
                    obuf[q, which] += part

        step(0, True)

        @pl.loop(1, GROUP // 4)
        def _(i):
            step(i, False)

    def begin_up():
        return remote(obuf.at[0, 0], cbuf.at[0, 0], bsend.at[0], brecv.at[0], y * NC + 1, x * NZ + up)

    def begin_down():
        return remote(obuf.at[0, 1], cbuf.at[1, 1], bsend.at[1], brecv.at[1], y * NC, x * NZ + down)

    def pass_down(q):
        slot, core = (q + 1, 0) if q < 3 else (4, 1)
        return remote(obuf.at[q], cbuf.at[slot], bsend.at[q + 1], brecv.at[slot], y * NC + core, x * NZ + down)

    def pass_up(q):
        return remote(obuf.at[q], cbuf.at[q + 1], bsend.at[q + 1], brecv.at[q + 1], y * NC + 1, x * NZ + up)

    for q in range(4):
        place(q)

        @pl.when(c == 0)
        def _():
            if q == 0:
                begin_up().start()
                begin_down().start()
            elif q == 1:
                begin_down().wait_recv()
                obuf[1, 1] += cbuf[1, 1]
                pass_down(1).start()
            else:
                pass_down(q - 1).wait_recv()
                obuf[q] += cbuf[q]
                pass_down(q).start()

        @pl.when(c == 1)
        def _():
            if q == 0:
                begin_up().wait_recv()
                obuf[0, 0] += cbuf[0, 0]
                pass_up(0).start()
            elif q < 3:
                pass_up(q - 1).wait_recv()
                obuf[q] += cbuf[q]
                pass_up(q).start()
            else:
                pass_up(2).wait_recv()
                pass_down(3).wait_recv()

    def to_strip(w):
        return remote(
            nbuf.at[pl.ds(pl.multiple_of(w * STRIP, 8), STRIP + 16)], fbuf.at[1 + y],
            nsend.at[w], frecv.at[1 + y], w, me_t,
        )

    def to_side(w, plane, t):
        return remote(
            nbuf.at[pl.ds(pl.multiple_of(w * STRIP + 8, 8), STRIP)], fbuf.at[plane, pl.ds(8, STRIP)],
            hsend.at[w], frecv.at[plane], w, t,
        )

    to_later = jnp.logical_and(y == NY - 1, me_t < last)
    to_earlier = jnp.logical_and(y == 0, me_t > 0)

    @pl.when(c == 1)
    def _():
        image = obuf[3, 0] + cbuf[3, 0] + cbuf[4, 0]
        light = obuf[3, 1] + cbuf[3, 1] + cbuf[4, 1]
        nbuf[pl.ds(0, 8)] = jnp.zeros((8, Y), F32)
        nbuf[pl.ds(X + 8, 8)] = jnp.zeros((8, Y), F32)
        nbuf[pl.ds(8, X)] = image / (1.0 + light)

        @pl.loop(1, NY * NC)
        def _(k):
            to_strip(lax.rem(me_w + k, NY * NC)).start()

        @pl.loop(0, NY * NC)
        def _(k):
            w = lax.rem(me_w + k, NY * NC)

            @pl.when(to_later)
            def _():
                to_side(w, 0, me_t + 1).start()

            @pl.when(to_earlier)
            def _():
                to_side(w, 5, me_t - 1).start()

        fbuf[1 + y] = nbuf[pl.ds(pl.multiple_of(me_w * STRIP, 8), STRIP + 16)]

    @pl.when(me_t == 0)
    def _():
        fbuf[0] = jnp.zeros((STRIP + 16, Y), F32)

    @pl.when(me_t == last)
    def _():
        fbuf[5] = jnp.zeros((STRIP + 16, Y), F32)

    for j in range(PLANES):

        @pl.when(jnp.logical_not(jnp.logical_and(c == 1, y == j)))
        def _():
            pltpu.make_async_copy(fbuf.at[1 + j], fbuf.at[1 + j], frecv.at[1 + j]).wait()

    @pl.when(me_t > 0)
    def _():
        pltpu.make_async_copy(fbuf.at[0, pl.ds(8, STRIP)], fbuf.at[0, pl.ds(8, STRIP)], frecv.at[0]).wait()

    @pl.when(me_t < last)
    def _():
        pltpu.make_async_copy(fbuf.at[5, pl.ds(8, STRIP)], fbuf.at[5, pl.ds(8, STRIP)], frecv.at[5]).wait()

    column = lax.broadcasted_iota(jnp.int32, (STRIP, Y), 1)
    for j in range(PLANES):
        center = fbuf[1 + j, pl.ds(8, STRIP)]
        beside = fbuf[j, pl.ds(8, STRIP)] + fbuf[2 + j, pl.ds(8, STRIP)]
        beside = beside + fbuf[1 + j, pl.ds(7, STRIP)] + fbuf[1 + j, pl.ds(9, STRIP)]
        before = jnp.where(column == 0, 0.0, pltpu.roll(center, 1, 1))
        after = jnp.where(column == Y - 1, 0.0, pltpu.roll(center, Y - 1, 1))
        out_ref[j] = beside + (before + after) - 6.0 * center

    pltpu.make_async_copy(sbuf.at[pl.ds(0, 124)], sbuf.at[pl.ds(0, 124)], asend).wait()
    pltpu.make_async_copy(cland.at[pl.ds(0, GROUP - 1)], cland.at[pl.ds(0, GROUP - 1)], csend).wait()

    @pl.when(c == 0)
    def _():
        begin_up().wait_send()
        begin_down().wait_send()
        for q in range(1, 4):
            pass_down(q).wait_send()

    @pl.when(c == 1)
    def _():
        for q in range(3):
            pass_up(q).wait_send()

        @pl.loop(1, NY * NC)
        def _(k):
            to_strip(lax.rem(me_w + k, NY * NC)).wait_send()

        @pl.loop(0, NY * NC)
        def _(k):
            w = lax.rem(me_w + k, NY * NC)

            @pl.when(to_later)
            def _():
                to_side(w, 0, me_t + 1).wait_send()

            @pl.when(to_earlier)
            def _():
                to_side(w, 5, me_t - 1).wait_send()


def per_device(source, receiver, corners):
    source = source.reshape(2, NX, NZ, PLANES, BX, BY)
    receiver = receiver.reshape(2, NX, NZ, PLANES, BX, BY)
    dma = pltpu.SemaphoreType.DMA
    return pl.pallas_call(
        kernel,
        out_shape=jax.ShapeDtypeStruct((PLANES, STRIP, Y), F32),
        in_specs=[
            pl.BlockSpec(memory_space=pltpu.SMEM),
            pl.BlockSpec(memory_space=pl.ANY),
            pl.BlockSpec(memory_space=pl.ANY),
        ],
        out_specs=pl.BlockSpec(memory_space=pltpu.VMEM),
        scratch_shapes=[
            pltpu.VMEM((NZ, 2, 2, NX, NY, BX, BY), BF16),
            pltpu.VMEM((NZ * NX * NY, 2, 2, BX, BY), BF16),
            pltpu.VMEM((4, GROUP, 2, 2, BX, BY), BF16),
            pltpu.VMEM((1, 128), jnp.int32),
            pltpu.VMEM((GROUP, 1, 128), jnp.int32),
            pltpu.VMEM((GROUP // 4, X, 256), BF16),
            pltpu.VMEM((GROUP // 4, 256, 128), BF16),
            pltpu.VMEM((4, 2, X, Y), F32),
            pltpu.VMEM((5, 2, X, Y), F32),
            pltpu.VMEM((X + 16, Y), F32),
            pltpu.VMEM((PLANES + 2, STRIP + 16, Y), F32),
            dma((NZ, 2)), dma, dma((4,)), dma, dma,
            dma((5,)), dma((5,)), dma((8,)), dma((8,)), dma((6,)),
        ],
        compiler_params=pltpu.CompilerParams(
            collective_id=0, has_side_effects=True, vmem_limit_bytes=48 << 20
        ),
        name="stack_shots",
    )(corners, source, receiver)


def solution(mesh):
    return jax.shard_map(
        per_device,
        mesh=mesh,
        in_specs=(
            P(("shot", "tile"), None, None, None, None),
            P(("shot", "tile"), None, None, None, None),
            P(("shot", "tile"), None),
        ),
        out_specs=P("tile", "shot", None),
        check_vma=False,
    )
```

```python
import functools

import jax
import jax.numpy as jnp
from jax import lax
from jax.experimental import pallas as pl
from jax.experimental.pallas import tpu as pltpu
from jax.sharding import PartitionSpec as P

MESH = pl.DeviceIdType.MESH
NX, NY, NZ, NC = 4, 4, 8, 2
GROUP = NX * NY * NC
PLANES = NY
X = 256
Y = 256
BX = 32
BY = 128
STRIP = 32
F32 = jnp.float32
BF16 = jnp.bfloat16

ORDER = (
    (1, 0), (0, 1), (3, 3), (2, 1), (0, 3), (1, 2), (3, 0), (2, 2),
    (1, 1), (0, 2), (3, 1), (2, 3), (1, 3), (3, 2), (2, 0), (0, 0),
)


def kernel(
    corners_hbm, src_hbm, rcv_hbm, out_ref,
    corners_ref, lbuf, sbuf, rbuf, cmsg, cland, rows, mask, obuf, cbuf, nbuf, fbuf,
    cornersem, lsem, asend, arecv, csend, crecv, bsend, brecv, nsend, hsend, frecv,
):
    me_w = lax.axis_index("shot")
    me_t = lax.axis_index("tile")
    y, c = me_w // NC, lax.rem(me_w, NC)
    x, z = me_t // NZ, lax.rem(me_t, NZ)
    me_g = x * (NY * NC) + me_w
    up, down = lax.rem(z + 1, NZ), lax.rem(z + NZ - 1, NZ)

    def chip(dx, dy):
        return lax.rem(x + dx, NX), lax.rem(y + dy, NY)

    def remote(src, dst, send, recv, w, t):
        return pltpu.make_async_remote_copy(
            src_ref=src, dst_ref=dst, send_sem=send, recv_sem=recv,
            device_id=(w, t), device_id_type=MESH,
        )

    def depth_of(k):
        half = k // 2
        step = jnp.where(lax.rem(k, 2) == 0, half + 4, 3 - half)
        return lax.rem(z + step, NZ)

    def load(k):
        zt = depth_of(k)
        return (
            pltpu.make_async_copy(src_hbm.at[:, :, zt], lbuf.at[k, 0], lsem.at[k, 0]),
            pltpu.make_async_copy(rcv_hbm.at[:, :, zt], lbuf.at[k, 1], lsem.at[k, 1]),
        )

    corners_copy = pltpu.make_async_copy(corners_hbm, corners_ref, cornersem)
    corners_copy.start()

    @pl.loop(0, NZ)
    def _(k):
        for copy in load(k):
            copy.start()

    barrier = pltpu.get_barrier_semaphore()

    def greet(w, t):
        pl.semaphore_signal(barrier, inc=1, device_id=(w, t), device_id_type=MESH)

    @pl.loop(1, GROUP)
    def _(g):
        other = lax.rem(me_g + g, GROUP)
        greet(lax.rem(other, NY * NC), (other // (NY * NC)) * NZ + z)

    for k in range(NC):
        greet(y * NC + k, x * NZ + up)
        greet(y * NC + k, x * NZ + down)
    last = NX * NZ - 1

    @pl.loop(0, NY * NC)
    def _(w):
        @pl.when(me_t > 0)
        def _():
            greet(w, me_t - 1)

        @pl.when(me_t < last)
        def _():
            greet(w, me_t + 1)

    corners_copy.wait()
    first_col = [corners_ref[k, 1] for k in range(2)]
    lane = lax.broadcasted_iota(jnp.int32, (1, 128), 1)
    a = lax.rem(lane, BX)
    cmsg[...] = jnp.where(
        lane < 32,
        corners_ref[0, 0] + a,
        jnp.where(
            lane < 64,
            corners_ref[1, 0] + a,
            jnp.where(lane < 96, first_col[0] + 0 * lane, first_col[1] + 0 * lane),
        ),
    )
    cland[me_g] = cmsg[...]
    edges = (me_t > 0).astype(jnp.int32) + (me_t < last).astype(jnp.int32)
    pl.semaphore_wait(barrier, GROUP - 1 + 2 * NC + NY * NC * edges)

    @pl.loop(1, GROUP)
    def _(g):
        other = lax.rem(me_g + g, GROUP)
        remote(
            cmsg, cland.at[me_g], csend, crecv,
            lax.rem(other, NY * NC), (other // (NY * NC)) * NZ + z,
        ).start()

    @pl.loop(0, NZ)
    def _(k):
        for copy in load(k):
            copy.wait()
        for which in range(2):
            for shot in range(2):
                block = lbuf[k, which, shot].reshape(NX * NY * BX, BY).astype(F32)
                block = pltpu.roll(block, lax.rem(first_col[shot], BY), 1).astype(BF16)
                sbuf[pl.ds(k * 16, 16), which, shot] = block.reshape(NX * NY, BX, BY)
        core, q = lax.rem(k, 2), k // 2
        for dx, dy in ORDER:
            tx, ty = chip(dx, dy)

            def send():
                remote(
                    sbuf.at[k * 16 + tx * NY + ty], rbuf.at[q, me_g], asend, arecv.at[q],
                    ty * NC + core, tx * NZ + z,
                ).start()

            if (dx, dy) == (0, 0):
                pl.when(core != c)(send)
            else:
                send()

        @pl.when(core == c)
        def _():
            rbuf[q, me_g] = sbuf[k * 16 + x * NY + y]

    pltpu.make_async_copy(cland.at[pl.ds(0, GROUP - 1)], cland.at[pl.ds(0, GROUP - 1)], crecv).wait()

    @pl.loop(0, GROUP // 4)
    def _(i):
        row = lax.broadcasted_iota(jnp.int32, (X, 128), 0)
        for h in range(2):
            one = cland[4 * i + 2 * h]
            two = cland[4 * i + 2 * h + 1]
            both = jnp.where(lane < 64, one, pltpu.roll(two, 64, 1))
            rows[i, :, pl.ds(h * 128, 128)] = (row == both).astype(F32).astype(BF16)
        wide = lax.broadcasted_iota(jnp.int32, (BX, 128), 1)
        for s in range(4):
            msg = cland[4 * i + s]
            for shot in range(2):
                col = msg[:, 64 + 32 * shot : 65 + 32 * shot]
                left = (wide >= col).astype(F32).astype(BF16)
                mask[i, pl.ds((2 * s + shot) * BX, BX), :] = left

    def place(q):
        pltpu.make_async_copy(
            rbuf.at[q, pl.ds(0, GROUP - 1)], rbuf.at[q, pl.ds(0, GROUP - 1)], arecv.at[q]
        ).wait()

        def step(i, fresh):
            got = rbuf[q, pl.ds(4 * i, 4)]
            wave = got[:, 0].reshape(256, BY).astype(F32)
            back = got[:, 1].reshape(256, BY).astype(F32)
            keep = mask[i]
            table = rows[i]
            for which, value in ((0, wave * back), (1, wave * wave)):
                hi = value.astype(BF16)
                lo = (value - hi.astype(F32)).astype(BF16)
                hi_left, lo_left = hi * keep, lo * keep
                hi_both = jnp.concatenate((hi_left, hi - hi_left), axis=1)
                lo_both = jnp.concatenate((lo_left, lo - lo_left), axis=1)
                part = jnp.dot(table, hi_both, preferred_element_type=F32)
                part = part + jnp.dot(table, lo_both, preferred_element_type=F32)
                if fresh:
                    obuf[q, which] = part
                else:
                    obuf[q, which] += part

        step(0, True)

        @pl.loop(1, GROUP // 4)
        def _(i):
            step(i, False)

    def begin_up():
        return remote(obuf.at[0, 0], cbuf.at[0, 0], bsend.at[0], brecv.at[0], y * NC + 1, x * NZ + up)

    def begin_down():
        return remote(obuf.at[0, 1], cbuf.at[1, 1], bsend.at[1], brecv.at[1], y * NC, x * NZ + down)

    def pass_down(q):
        slot, core = (q + 1, 0) if q < 3 else (4, 1)
        return remote(obuf.at[q], cbuf.at[slot], bsend.at[q + 1], brecv.at[slot], y * NC + core, x * NZ + down)

    def pass_up(q):
        return remote(obuf.at[q], cbuf.at[q + 1], bsend.at[q + 1], brecv.at[q + 1], y * NC + 1, x * NZ + up)

    for q in range(4):
        place(q)

        @pl.when(c == 0)
        def _():
            if q == 0:
                begin_up().start()
                begin_down().start()
            elif q == 1:
                begin_down().wait_recv()
                obuf[1, 1] += cbuf[1, 1]
                pass_down(1).start()
            else:
                pass_down(q - 1).wait_recv()
                obuf[q] += cbuf[q]
                pass_down(q).start()

        @pl.when(c == 1)
        def _():
            if q == 0:
                begin_up().wait_recv()
                obuf[0, 0] += cbuf[0, 0]
                pass_up(0).start()
            elif q < 3:
                pass_up(q - 1).wait_recv()
                obuf[q] += cbuf[q]
                pass_up(q).start()
            else:
                pass_up(2).wait_recv()
                pass_down(3).wait_recv()

    def to_strip(w):
        return remote(
            nbuf.at[pl.ds(pl.multiple_of(w * STRIP, 8), STRIP + 16)], fbuf.at[1 + y],
            nsend.at[w], frecv.at[1 + y], w, me_t,
        )

    def to_side(w, plane, t):
        return remote(
            nbuf.at[pl.ds(pl.multiple_of(w * STRIP + 8, 8), STRIP)], fbuf.at[plane, pl.ds(8, STRIP)],
            hsend.at[w], frecv.at[plane], w, t,
        )

    to_later = jnp.logical_and(y == NY - 1, me_t < last)
    to_earlier = jnp.logical_and(y == 0, me_t > 0)

    @pl.when(c == 1)
    def _():
        image = obuf[3, 0] + cbuf[3, 0] + cbuf[4, 0]
        light = obuf[3, 1] + cbuf[3, 1] + cbuf[4, 1]
        nbuf[pl.ds(0, 8)] = jnp.zeros((8, Y), F32)
        nbuf[pl.ds(X + 8, 8)] = jnp.zeros((8, Y), F32)
        nbuf[pl.ds(8, X)] = image / (1.0 + light)

        @pl.loop(1, NY * NC)
        def _(k):
            to_strip(lax.rem(me_w + k, NY * NC)).start()

        @pl.loop(0, NY * NC)
        def _(k):
            w = lax.rem(me_w + k, NY * NC)

            @pl.when(to_later)
            def _():
                to_side(w, 0, me_t + 1).start()

            @pl.when(to_earlier)
            def _():
                to_side(w, 5, me_t - 1).start()

        fbuf[1 + y] = nbuf[pl.ds(pl.multiple_of(me_w * STRIP, 8), STRIP + 16)]

    @pl.when(me_t == 0)
    def _():
        fbuf[0] = jnp.zeros((STRIP + 16, Y), F32)

    @pl.when(me_t == last)
    def _():
        fbuf[5] = jnp.zeros((STRIP + 16, Y), F32)

    for j in range(PLANES):

        @pl.when(jnp.logical_not(jnp.logical_and(c == 1, y == j)))
        def _():
            pltpu.make_async_copy(fbuf.at[1 + j], fbuf.at[1 + j], frecv.at[1 + j]).wait()

    @pl.when(me_t > 0)
    def _():
        pltpu.make_async_copy(fbuf.at[0, pl.ds(8, STRIP)], fbuf.at[0, pl.ds(8, STRIP)], frecv.at[0]).wait()

    @pl.when(me_t < last)
    def _():
        pltpu.make_async_copy(fbuf.at[5, pl.ds(8, STRIP)], fbuf.at[5, pl.ds(8, STRIP)], frecv.at[5]).wait()

    column = lax.broadcasted_iota(jnp.int32, (STRIP, Y), 1)
    for j in range(PLANES):
        center = fbuf[1 + j, pl.ds(8, STRIP)]
        beside = fbuf[j, pl.ds(8, STRIP)] + fbuf[2 + j, pl.ds(8, STRIP)]
        beside = beside + fbuf[1 + j, pl.ds(7, STRIP)] + fbuf[1 + j, pl.ds(9, STRIP)]
        before = jnp.where(column == 0, 0.0, pltpu.roll(center, 1, 1))
        after = jnp.where(column == Y - 1, 0.0, pltpu.roll(center, Y - 1, 1))
        out_ref[j] = beside + (before + after) - 6.0 * center

    pltpu.make_async_copy(sbuf.at[pl.ds(0, 124)], sbuf.at[pl.ds(0, 124)], asend).wait()
    pltpu.make_async_copy(cland.at[pl.ds(0, GROUP - 1)], cland.at[pl.ds(0, GROUP - 1)], csend).wait()

    @pl.when(c == 0)
    def _():
        begin_up().wait_send()
        begin_down().wait_send()
        for q in range(1, 4):
            pass_down(q).wait_send()

    @pl.when(c == 1)
    def _():
        for q in range(3):
            pass_up(q).wait_send()

        @pl.loop(1, NY * NC)
        def _(k):
            to_strip(lax.rem(me_w + k, NY * NC)).wait_send()

        @pl.loop(0, NY * NC)
        def _(k):
            w = lax.rem(me_w + k, NY * NC)

            @pl.when(to_later)
            def _():
                to_side(w, 0, me_t + 1).wait_send()

            @pl.when(to_earlier)
            def _():
                to_side(w, 5, me_t - 1).wait_send()


def per_device(source, receiver, corners):
    source = source.reshape(2, NX, NZ, PLANES, BX, BY)
    receiver = receiver.reshape(2, NX, NZ, PLANES, BX, BY)
    dma = pltpu.SemaphoreType.DMA
    return pl.pallas_call(
        kernel,
        out_shape=jax.ShapeDtypeStruct((PLANES, STRIP, Y), F32),
        in_specs=[
            pl.BlockSpec(memory_space=pltpu.HBM),
            pl.BlockSpec(memory_space=pltpu.HBM),
            pl.BlockSpec(memory_space=pltpu.HBM),
        ],
        out_specs=pl.BlockSpec(memory_space=pltpu.VMEM),
        scratch_shapes=[
            pltpu.SMEM((2, 2), jnp.int32),
            pltpu.VMEM((NZ, 2, 2, NX, NY, BX, BY), BF16),
            pltpu.VMEM((NZ * NX * NY, 2, 2, BX, BY), BF16),
            pltpu.VMEM((4, GROUP, 2, 2, BX, BY), BF16),
            pltpu.VMEM((1, 128), jnp.int32),
            pltpu.VMEM((GROUP, 1, 128), jnp.int32),
            pltpu.VMEM((GROUP // 4, X, 256), BF16),
            pltpu.VMEM((GROUP // 4, 256, 128), BF16),
            pltpu.VMEM((4, 2, X, Y), F32),
            pltpu.VMEM((5, 2, X, Y), F32),
            pltpu.VMEM((X + 16, Y), F32),
            pltpu.VMEM((PLANES + 2, STRIP + 16, Y), F32),
            dma, dma((NZ, 2)), dma, dma((4,)), dma, dma,
            dma((5,)), dma((5,)), dma((8,)), dma((8,)), dma((6,)),
        ],
        compiler_params=pltpu.CompilerParams(
            collective_id=0, has_side_effects=True, vmem_limit_bytes=67043328
        ),
        name="stack_shots",
    )(corners, source, receiver)


def solution(mesh):
    return jax.shard_map(
        per_device,
        mesh=mesh,
        in_specs=(
            P(("shot", "tile"), None, None, None, None),
            P(("shot", "tile"), None, None, None, None),
            P(("shot", "tile"), None),
        ),
        out_specs=P("tile", "shot", None),
        check_vma=False,
    )
```

```python
import functools

import jax
import jax.numpy as jnp
from jax import lax
from jax.experimental import pallas as pl
from jax.experimental.pallas import tpu as pltpu
from jax.sharding import PartitionSpec as P

MESH = pl.DeviceIdType.MESH
NX, NY, NZ, NC = 4, 4, 8, 2
GROUP = NX * NY * NC
BLOCKS = GROUP // 4
PLANES = NY
X = 256
Y = 256
BX = 32
BY = 128
STRIP = 32
F32 = jnp.float32
BF16 = jnp.bfloat16

ORDER = (
    (1, 0), (0, 1), (3, 3), (2, 1), (0, 3), (1, 2), (3, 0), (2, 2),
    (1, 1), (0, 2), (3, 1), (2, 3), (1, 3), (3, 2), (2, 0), (0, 0),
)


def kernel(
    corners_hbm, src_hbm, rcv_hbm, out_ref,
    corners_ref, lbuf, head_out, sbuf, head_in, rbuf, rows, mask, obuf, cbuf, nbuf, fbuf,
    cornersem, lsem, headsend, asend, arecv, bsend, brecv, nsend, hsend, frecv,
):
    me_w = lax.axis_index("shot")
    me_t = lax.axis_index("tile")
    y, c = me_w // NC, lax.rem(me_w, NC)
    x, z = me_t // NZ, lax.rem(me_t, NZ)
    me_g = x * (NY * NC) + me_w
    me_slot = 2 * (NX * NY - 1) + c
    up, down = lax.rem(z + 1, NZ), lax.rem(z + NZ - 1, NZ)

    def chip(dx, dy):
        return lax.rem(x + dx, NX), lax.rem(y + dy, NY)

    def remote(src, dst, send, recv, w, t):
        return pltpu.make_async_remote_copy(
            src_ref=src, dst_ref=dst, send_sem=send, recv_sem=recv,
            device_id=(w, t), device_id_type=MESH,
        )

    def depth_of(k):
        half = k // 2
        step = jnp.where(lax.rem(k, 2) == 0, half + 4, 3 - half)
        return lax.rem(z + step, NZ)

    def load(k):
        zt = depth_of(k)
        return (
            pltpu.make_async_copy(src_hbm.at[:, :, zt], lbuf.at[k, 0], lsem.at[k, 0]),
            pltpu.make_async_copy(rcv_hbm.at[:, :, zt], lbuf.at[k, 1], lsem.at[k, 1]),
        )

    barrier = pltpu.get_barrier_semaphore()

    def greet(w, t):
        pl.semaphore_signal(barrier, inc=1, device_id=(w, t), device_id_type=MESH)

    @pl.loop(1, GROUP)
    def _(g):
        other = lax.rem(me_g + g, GROUP)
        greet(lax.rem(other, NY * NC), (other // (NY * NC)) * NZ + z)

    for k in range(NC):
        greet(y * NC + k, x * NZ + up)
        greet(y * NC + k, x * NZ + down)
    last = NX * NZ - 1

    @pl.loop(0, NY * NC)
    def _(w):
        @pl.when(me_t > 0)
        def _():
            greet(w, me_t - 1)

        @pl.when(me_t < last)
        def _():
            greet(w, me_t + 1)

    corners_copy = pltpu.make_async_copy(corners_hbm, corners_ref, cornersem)
    corners_copy.start()

    @pl.loop(0, NZ)
    def _(k):
        for copy in load(k):
            copy.start()

    corners_copy.wait()
    first_col = [corners_ref[k, 1] for k in range(2)]
    lane = lax.broadcasted_iota(jnp.int32, (8, 128), 1)
    a = lax.rem(lane, BX)
    note = jnp.where(
        lane < 32,
        corners_ref[0, 0] + a,
        jnp.where(
            lane < 64,
            corners_ref[1, 0] + a,
            jnp.where(lane < 96, first_col[0] + 0 * lane, first_col[1] + 0 * lane),
        ),
    )
    note = note.astype(F32).astype(BF16)

    def turn(k, out, at):
        for copy in load(k):
            copy.wait()
        for which in range(2):
            for shot in range(2):
                block = lbuf[k, which, shot].reshape(NX * NY * BX, BY).astype(F32)
                block = pltpu.roll(block, lax.rem(first_col[shot], BY), 1).astype(BF16)
                out[pl.ds(at, 16), pl.ds(64 * which + 32 * shot, BX)] = block.reshape(NX * NY, BX, BY)

    def send(k, out, into, sem, q):
        core = lax.rem(k, 2)
        for p, (dx, dy) in enumerate(ORDER):
            tx, ty = chip(dx, dy)
            copy = remote(
                out(tx * NY + ty), into(2 * p + c), sem, arecv.at[q, p // 2],
                ty * NC + core, tx * NZ + z,
            )
            if (dx, dy) == (0, 0):
                pl.when(core != c)(copy.start)
            else:
                copy.start()

    for k in range(2):
        turn(k, head_out, 16 * k)
        for h in range(16):
            head_out[16 * k + h, pl.ds(128, 8)] = note

        @pl.when(c == k)
        def _():
            head_in[me_slot, pl.ds(0, 136)] = head_out[16 * k + x * NY + y, pl.ds(0, 136)]

    edges = (me_t > 0).astype(jnp.int32) + (me_t < last).astype(jnp.int32)
    pl.semaphore_wait(barrier, GROUP - 1 + 2 * NC + NY * NC * edges)

    for k in range(2):
        send(
            k,
            lambda chip: head_out.at[16 * k + chip, pl.ds(0, 136)],
            lambda slot: head_in.at[slot, pl.ds(0, 136)],
            headsend,
            0,
        )

    @pl.loop(2, NZ)
    def _(k):
        q = k // 2
        at = (k - 2) * 16
        turn(k, sbuf, at)
        send(k, lambda chip: sbuf.at[at + chip], lambda slot: rbuf.at[q - 1, slot], asend, q)

        @pl.when(lax.rem(k, 2) == c)
        def _():
            rbuf[q - 1, me_slot] = sbuf[at + x * NY + y]

    def tables(i):
        row = lax.broadcasted_iota(jnp.int32, (X, 128), 0)
        wide = lax.broadcasted_iota(jnp.int32, (BX, 128), 1)
        first = wide[0:1]
        notes = [head_in[4 * i + s, pl.ds(128, 8)].astype(F32)[0:1].astype(jnp.int32) for s in range(4)]
        for h in range(2):
            both = jnp.where(first < 64, notes[2 * h], pltpu.roll(notes[2 * h + 1], 64, 1))
            rows[i, :, pl.ds(h * 128, 128)] = (row == both).astype(F32).astype(BF16)
        for s in range(4):
            for shot in range(2):
                col = notes[s][:, 64 + 32 * shot : 65 + 32 * shot]
                left = (wide >= col).astype(F32).astype(BF16)
                mask[i, pl.ds((2 * s + shot) * BX, BX), :] = left

    def place(q):
        def arrive(i, count):
            if q == 0:
                part = head_in.at[pl.ds(0, count), pl.ds(0, 136)]
            else:
                part = rbuf.at[q - 1, pl.ds(0, count)]
            pltpu.make_async_copy(part, part, arecv.at[q, i]).wait()

        def step(i, fresh):
            if q == 0:
                tables(i)
            got = head_in[pl.ds(4 * i, 4)] if q == 0 else rbuf[q - 1, pl.ds(4 * i, 4)]
            wave = got[:, 0:64].reshape(256, BY).astype(F32)
            back = got[:, 64:128].reshape(256, BY).astype(F32)
            keep = mask[i]
            table = rows[i]
            for which, value in ((0, wave * back), (1, wave * wave)):
                hi = value.astype(BF16)
                lo = (value - hi.astype(F32)).astype(BF16)
                hi_left, lo_left = hi * keep, lo * keep
                hi_both = jnp.concatenate((hi_left, hi - hi_left), axis=1)
                lo_both = jnp.concatenate((lo_left, lo - lo_left), axis=1)
                part = jnp.dot(table, hi_both, preferred_element_type=F32)
                part = part + jnp.dot(table, lo_both, preferred_element_type=F32)
                if fresh:
                    obuf[q, which] = part
                else:
                    obuf[q, which] += part

        arrive(0, 4)
        step(0, True)

        @pl.loop(1, BLOCKS - 1)
        def _(i):
            arrive(i, 4)
            step(i, False)

        arrive(BLOCKS - 1, 3)
        step(BLOCKS - 1, False)

    def begin_up():
        return remote(obuf.at[0, 0], cbuf.at[0, 0], bsend.at[0], brecv.at[0], y * NC + 1, x * NZ + up)

    def begin_down():
        return remote(obuf.at[0, 1], cbuf.at[1, 1], bsend.at[1], brecv.at[1], y * NC, x * NZ + down)

    def pass_down(q):
        return remote(obuf.at[q], cbuf.at[q + 1], bsend.at[q + 1], brecv.at[q + 1], y * NC, x * NZ + down)

    def last_down(p):
        part = pl.ds(64 * p, 64)
        return tuple(
            remote(
                obuf.at[3, h, part], cbuf.at[4, h, part], bsend.at[4 + 2 * p + h], brecv.at[4 + 2 * p + h],
                y * NC + 1, x * NZ + down,
            )
            for h in range(2)
        )

    def pass_up(q):
        return remote(obuf.at[q], cbuf.at[q + 1], bsend.at[q + 1], brecv.at[q + 1], y * NC + 1, x * NZ + up)

    for q in range(4):
        place(q)

        @pl.when(c == 0)
        def _():
            if q == 0:
                begin_up().start()
                begin_down().start()
            elif q == 1:
                begin_down().wait_recv()
                obuf[1, 1] += cbuf[1, 1]
                pass_down(1).start()
            else:
                pass_down(q - 1).wait_recv()
                if q < 3:
                    obuf[q] += cbuf[q]
                    pass_down(q).start()
                else:
                    for p in range(4):
                        part = pl.ds(64 * p, 64)
                        obuf[3, :, part] += cbuf[3, :, part]
                        for copy in last_down(p):
                            copy.start()

        @pl.when(c == 1)
        def _():
            if q == 0:
                begin_up().wait_recv()
                obuf[0, 0] += cbuf[0, 0]
                pass_up(0).start()
            elif q < 3:
                pass_up(q - 1).wait_recv()
                obuf[q] += cbuf[q]
                pass_up(q).start()
            else:
                pass_up(2).wait_recv()

    def to_strip(w):
        return remote(
            nbuf.at[pl.ds(pl.multiple_of(w * STRIP, 8), STRIP + 16)], fbuf.at[1 + y],
            nsend.at[w], frecv.at[1 + y], w, me_t,
        )

    def to_side(w, plane, t):
        return remote(
            nbuf.at[pl.ds(pl.multiple_of(w * STRIP + 8, 8), STRIP)], fbuf.at[plane, pl.ds(8, STRIP)],
            hsend.at[w], frecv.at[plane], w, t,
        )

    to_later = jnp.logical_and(y == NY - 1, me_t < last)
    to_earlier = jnp.logical_and(y == 0, me_t > 0)

    @pl.when(c == 1)
    def _():
        nbuf[pl.ds(0, 8)] = jnp.zeros((8, Y), F32)
        nbuf[pl.ds(X + 8, 8)] = jnp.zeros((8, Y), F32)
        for p in range(4):
            for copy in last_down(p):
                copy.wait_recv()
            part = pl.ds(64 * p, 64)
            image = obuf[3, 0, part] + cbuf[3, 0, part] + cbuf[4, 0, part]
            light = obuf[3, 1, part] + cbuf[3, 1, part] + cbuf[4, 1, part]
            nbuf[pl.ds(64 * p + 8, 64)] = image / (1.0 + light)

        @pl.loop(1, NY * NC)
        def _(k):
            to_strip(lax.rem(me_w + k, NY * NC)).start()

        @pl.loop(0, NY * NC)
        def _(w):
            @pl.when(to_later)
            def _():
                to_side(w, 0, me_t + 1).start()

            @pl.when(to_earlier)
            def _():
                to_side(w, 5, me_t - 1).start()

        fbuf[1 + y] = nbuf[pl.ds(pl.multiple_of(me_w * STRIP, 8), STRIP + 16)]

    @pl.when(me_t == 0)
    def _():
        fbuf[0] = jnp.zeros((STRIP + 16, Y), F32)

    @pl.when(me_t == last)
    def _():
        fbuf[5] = jnp.zeros((STRIP + 16, Y), F32)

    for j in range(PLANES):

        @pl.when(jnp.logical_not(jnp.logical_and(c == 1, y == j)))
        def _():
            pltpu.make_async_copy(fbuf.at[1 + j], fbuf.at[1 + j], frecv.at[1 + j]).wait()

    @pl.when(me_t > 0)
    def _():
        pltpu.make_async_copy(fbuf.at[0, pl.ds(8, STRIP)], fbuf.at[0, pl.ds(8, STRIP)], frecv.at[0]).wait()

    @pl.when(me_t < last)
    def _():
        pltpu.make_async_copy(fbuf.at[5, pl.ds(8, STRIP)], fbuf.at[5, pl.ds(8, STRIP)], frecv.at[5]).wait()

    column = lax.broadcasted_iota(jnp.int32, (STRIP, Y), 1)
    for j in range(PLANES):
        center = fbuf[1 + j, pl.ds(8, STRIP)]
        beside = fbuf[j, pl.ds(8, STRIP)] + fbuf[2 + j, pl.ds(8, STRIP)]
        beside = beside + fbuf[1 + j, pl.ds(7, STRIP)] + fbuf[1 + j, pl.ds(9, STRIP)]
        before = jnp.where(column == 0, 0.0, pltpu.roll(center, 1, 1))
        after = jnp.where(column == Y - 1, 0.0, pltpu.roll(center, Y - 1, 1))
        out_ref[j] = beside + (before + after) - 6.0 * center

    for part, sem in ((head_out.at[pl.ds(0, 31), pl.ds(0, 136)], headsend), (sbuf.at[pl.ds(0, 93)], asend)):
        pltpu.make_async_copy(part, part, sem).wait()

    @pl.when(c == 0)
    def _():
        begin_up().wait_send()
        begin_down().wait_send()
        for q in range(1, 3):
            pass_down(q).wait_send()
        for p in range(4):
            for copy in last_down(p):
                copy.wait_send()

    @pl.when(c == 1)
    def _():
        for q in range(3):
            pass_up(q).wait_send()
        @pl.loop(1, NY * NC)
        def _(k):
            to_strip(lax.rem(me_w + k, NY * NC)).wait_send()

        @pl.loop(0, NY * NC)
        def _(w):
            @pl.when(to_later)
            def _():
                to_side(w, 0, me_t + 1).wait_send()

            @pl.when(to_earlier)
            def _():
                to_side(w, 5, me_t - 1).wait_send()


def per_device(source, receiver, corners):
    source = source.reshape(2, NX, NZ, PLANES, BX, BY)
    receiver = receiver.reshape(2, NX, NZ, PLANES, BX, BY)
    dma = pltpu.SemaphoreType.DMA
    return pl.pallas_call(
        kernel,
        out_shape=jax.ShapeDtypeStruct((PLANES, STRIP, Y), F32),
        in_specs=[
            pl.BlockSpec(memory_space=pltpu.HBM),
            pl.BlockSpec(memory_space=pltpu.HBM),
            pl.BlockSpec(memory_space=pltpu.HBM),
        ],
        out_specs=pl.BlockSpec(memory_space=pltpu.VMEM),
        scratch_shapes=[
            pltpu.SMEM((2, 2), jnp.int32),
            pltpu.VMEM((NZ, 2, 2, NX, NY, BX, BY), BF16),
            pltpu.VMEM((2 * NX * NY, 144, BY), BF16),
            pltpu.VMEM((6 * NX * NY, 128, BY), BF16),
            pltpu.VMEM((GROUP, 144, BY), BF16),
            pltpu.VMEM((3, GROUP, 128, BY), BF16),
            pltpu.VMEM((BLOCKS, X, 256), BF16),
            pltpu.VMEM((BLOCKS, 256, 128), BF16),
            pltpu.VMEM((4, 2, X, Y), F32),
            pltpu.VMEM((5, 2, X, Y), F32),
            pltpu.VMEM((X + 16, Y), F32),
            pltpu.VMEM((PLANES + 2, STRIP + 16, Y), F32),
            dma, dma((NZ, 2)), dma, dma, dma((4, BLOCKS)),
            dma((12,)), dma((12,)), dma((8,)), dma((8,)), dma((6,)),
        ],
        compiler_params=pltpu.CompilerParams(
            collective_id=0, has_side_effects=True, vmem_limit_bytes=67043328
        ),
        name="stack_shots",
    )(corners, source, receiver)


def solution(mesh):
    return jax.shard_map(
        per_device,
        mesh=mesh,
        in_specs=(
            P(("shot", "tile"), None, None, None, None),
            P(("shot", "tile"), None, None, None, None),
            P(("shot", "tile"), None),
        ),
        out_specs=P("tile", "shot", None),
        check_vma=False,
    )
```

```python
import functools

import jax
import jax.numpy as jnp
from jax import lax
from jax.experimental import pallas as pl
from jax.experimental.pallas import tpu as pltpu
from jax.sharding import PartitionSpec as P

MESH = pl.DeviceIdType.MESH
NX, NY, NZ, NC = 4, 4, 8, 2
GROUP = NX * NY * NC
BLOCKS = GROUP // 4
PLANES = NY
X = 256
Y = 256
BX = 32
BY = 128
STRIP = 32
F32 = jnp.float32
BF16 = jnp.bfloat16

ORDER = (
    (1, 0), (0, 1), (3, 3), (2, 1), (0, 3), (1, 2), (3, 0), (2, 2),
    (1, 1), (0, 2), (3, 1), (2, 3), (1, 3), (3, 2), (2, 0), (0, 0),
)


def kernel(
    corners_hbm, src_hbm, rcv_hbm, out_ref,
    corners_ref, lbuf, head_out, sbuf, head_in, rbuf, rows, mask, obuf, cbuf, nbuf, fbuf,
    cornersem, lsem, headsend, asend, arecv, bsend, brecv, nsend, hsend, frecv,
):
    me_w = lax.axis_index("shot")
    me_t = lax.axis_index("tile")
    y, c = me_w // NC, lax.rem(me_w, NC)
    x, z = me_t // NZ, lax.rem(me_t, NZ)
    me_g = x * (NY * NC) + me_w
    me_slot = 2 * (NX * NY - 1) + c
    up, down = lax.rem(z + 1, NZ), lax.rem(z + NZ - 1, NZ)

    def chip(dx, dy):
        return lax.rem(x + dx, NX), lax.rem(y + dy, NY)

    def remote(src, dst, send, recv, w, t):
        return pltpu.make_async_remote_copy(
            src_ref=src, dst_ref=dst, send_sem=send, recv_sem=recv,
            device_id=(w, t), device_id_type=MESH,
        )

    def depth_of(k):
        half = k // 2
        step = jnp.where(lax.rem(k, 2) == 0, half + 4, 3 - half)
        return lax.rem(z + step, NZ)

    def load(k):
        zt = depth_of(k)
        return (
            pltpu.make_async_copy(src_hbm.at[:, :, zt], lbuf.at[k, 0], lsem.at[k, 0]),
            pltpu.make_async_copy(rcv_hbm.at[:, :, zt], lbuf.at[k, 1], lsem.at[k, 1]),
        )

    barrier = pltpu.get_barrier_semaphore()

    def greet(w, t):
        pl.semaphore_signal(barrier, inc=1, device_id=(w, t), device_id_type=MESH)

    @pl.loop(1, GROUP)
    def _(g):
        other = lax.rem(me_g + g, GROUP)
        greet(lax.rem(other, NY * NC), (other // (NY * NC)) * NZ + z)

    for k in range(NC):
        greet(y * NC + k, x * NZ + up)
        greet(y * NC + k, x * NZ + down)
    last = NX * NZ - 1

    @pl.loop(0, NY * NC)
    def _(w):
        @pl.when(me_t > 0)
        def _():
            greet(w, me_t - 1)

        @pl.when(me_t < last)
        def _():
            greet(w, me_t + 1)

    corners_copy = pltpu.make_async_copy(corners_hbm, corners_ref, cornersem)
    corners_copy.start()

    @pl.loop(0, NZ)
    def _(k):
        for copy in load(k):
            copy.start()

    corners_copy.wait()
    first_col = [corners_ref[k, 1] for k in range(2)]
    lane = lax.broadcasted_iota(jnp.int32, (8, 128), 1)
    a = lax.rem(lane, BX)
    note = jnp.where(
        lane < 32,
        corners_ref[0, 0] + a,
        jnp.where(
            lane < 64,
            corners_ref[1, 0] + a,
            jnp.where(lane < 96, first_col[0] + 0 * lane, first_col[1] + 0 * lane),
        ),
    )
    note = note.astype(F32).astype(BF16)

    def turn(k, out, at):
        for copy in load(k):
            copy.wait()
        for which in range(2):
            for shot in range(2):
                block = lbuf[k, which, shot].reshape(NX * NY * BX, BY).astype(F32)
                block = pltpu.roll(block, lax.rem(first_col[shot], BY), 1).astype(BF16)
                out[pl.ds(at, 16), pl.ds(64 * which + 32 * shot, BX)] = block.reshape(NX * NY, BX, BY)

    def send(k, out, into, sem, q):
        core = lax.rem(k, 2)
        for p, (dx, dy) in enumerate(ORDER):
            tx, ty = chip(dx, dy)
            copy = remote(
                out(tx * NY + ty), into(2 * p + c), sem, arecv.at[q, p // 2],
                ty * NC + core, tx * NZ + z,
            )
            if (dx, dy) == (0, 0):
                pl.when(core != c)(copy.start)
            else:
                copy.start()

    for k in range(2):
        turn(k, head_out, 16 * k)
        for h in range(16):
            head_out[16 * k + h, pl.ds(128, 8)] = note

        @pl.when(c == k)
        def _():
            head_in[me_slot, pl.ds(0, 136)] = head_out[16 * k + x * NY + y, pl.ds(0, 136)]

    edges = (me_t > 0).astype(jnp.int32) + (me_t < last).astype(jnp.int32)
    pl.semaphore_wait(barrier, GROUP - 1 + 2 * NC + NY * NC * edges)

    for k in range(2):
        send(
            k,
            lambda chip: head_out.at[16 * k + chip, pl.ds(0, 136)],
            lambda slot: head_in.at[slot, pl.ds(0, 136)],
            headsend,
            0,
        )

    @pl.loop(2, NZ)
    def _(k):
        q = k // 2
        at = (k - 2) * 16
        turn(k, sbuf, at)
        send(k, lambda chip: sbuf.at[at + chip], lambda slot: rbuf.at[q - 1, slot], asend, q)

        @pl.when(lax.rem(k, 2) == c)
        def _():
            rbuf[q - 1, me_slot] = sbuf[at + x * NY + y]

    def tables(i):
        row = lax.broadcasted_iota(jnp.int32, (X, 128), 0)
        wide = lax.broadcasted_iota(jnp.int32, (BX, 128), 1)
        first = wide[0:1]
        notes = [head_in[4 * i + s, pl.ds(128, 8)].astype(F32)[0:1].astype(jnp.int32) for s in range(4)]
        for h in range(2):
            both = jnp.where(first < 64, notes[2 * h], pltpu.roll(notes[2 * h + 1], 64, 1))
            rows[i, :, pl.ds(h * 128, 128)] = (row == both).astype(F32).astype(BF16)
        for s in range(4):
            for shot in range(2):
                col = notes[s][:, 64 + 32 * shot : 65 + 32 * shot]
                left = (wide >= col).astype(F32).astype(BF16)
                mask[i, pl.ds((2 * s + shot) * BX, BX), :] = left

    def place(q):
        def arrive(i, count):
            if q == 0:
                part = head_in.at[pl.ds(0, count), pl.ds(0, 136)]
            else:
                part = rbuf.at[q - 1, pl.ds(0, count)]
            pltpu.make_async_copy(part, part, arecv.at[q, i]).wait()

        def step(i, fresh):
            if q == 0:
                tables(i)
            got = head_in[pl.ds(4 * i, 4)] if q == 0 else rbuf[q - 1, pl.ds(4 * i, 4)]
            wave = got[:, 0:64].reshape(256, BY).astype(F32)
            back = got[:, 64:128].reshape(256, BY).astype(F32)
            keep = mask[i]
            table = rows[i]
            for which, value in ((0, wave * back), (1, wave * wave)):
                hi = value.astype(BF16)
                lo = (value - hi.astype(F32)).astype(BF16)
                hi_left, lo_left = hi * keep, lo * keep
                hi_both = jnp.concatenate((hi_left, hi - hi_left), axis=1)
                lo_both = jnp.concatenate((lo_left, lo - lo_left), axis=1)
                part = jnp.dot(table, hi_both, preferred_element_type=F32)
                part = part + jnp.dot(table, lo_both, preferred_element_type=F32)
                if fresh:
                    obuf[q, which] = part
                else:
                    obuf[q, which] += part

        arrive(0, 4)
        step(0, True)

        @pl.loop(1, BLOCKS - 1)
        def _(i):
            arrive(i, 4)
            step(i, False)

        arrive(BLOCKS - 1, 3)
        step(BLOCKS - 1, False)

    def begin_up():
        return remote(obuf.at[0, 0], cbuf.at[0, 0], bsend.at[0], brecv.at[0], y * NC + 1, x * NZ + up)

    def begin_down():
        return remote(obuf.at[0, 1], cbuf.at[1, 1], bsend.at[1], brecv.at[1], y * NC, x * NZ + down)

    def pass_down(q):
        return remote(obuf.at[q], cbuf.at[q + 1], bsend.at[q + 1], brecv.at[q + 1], y * NC, x * NZ + down)

    def last_down(p):
        part = pl.ds(64 * p, 64)
        return tuple(
            remote(
                obuf.at[3, h, part], cbuf.at[4, h, part], bsend.at[4 + 2 * p + h], brecv.at[4 + 2 * p + h],
                y * NC + 1, x * NZ + down,
            )
            for h in range(2)
        )

    def pass_up(q):
        return remote(obuf.at[q], cbuf.at[q + 1], bsend.at[q + 1], brecv.at[q + 1], y * NC + 1, x * NZ + up)

    for q in range(4):
        place(q)

        @pl.when(c == 0)
        def _():
            if q == 0:
                begin_up().start()
                begin_down().start()
            elif q == 1:
                begin_down().wait_recv()
                obuf[1, 1] += cbuf[1, 1]
                pass_down(1).start()
            else:
                pass_down(q - 1).wait_recv()
                if q < 3:
                    obuf[q] += cbuf[q]
                    pass_down(q).start()
                else:
                    for p in range(4):
                        part = pl.ds(64 * p, 64)
                        obuf[3, :, part] += cbuf[3, :, part]
                        for copy in last_down(p):
                            copy.start()

        @pl.when(c == 1)
        def _():
            if q == 0:
                begin_up().wait_recv()
                obuf[0, 0] += cbuf[0, 0]
                pass_up(0).start()
            elif q < 3:
                pass_up(q - 1).wait_recv()
                obuf[q] += cbuf[q]
                pass_up(q).start()
            else:
                pass_up(2).wait_recv()

    def to_strip(w):
        return remote(
            nbuf.at[pl.ds(pl.multiple_of(w * STRIP, 8), STRIP + 16)], fbuf.at[1 + y],
            nsend.at[w], frecv.at[1 + y], w, me_t,
        )

    def to_side(w, plane, t):
        return remote(
            nbuf.at[pl.ds(pl.multiple_of(w * STRIP + 8, 8), STRIP)], fbuf.at[plane, pl.ds(8, STRIP)],
            hsend.at[w], frecv.at[plane], w, t,
        )

    to_later = jnp.logical_and(y == NY - 1, me_t < last)
    to_earlier = jnp.logical_and(y == 0, me_t > 0)

    @pl.when(c == 1)
    def _():
        nbuf[pl.ds(0, 8)] = jnp.zeros((8, Y), F32)
        nbuf[pl.ds(X + 8, 8)] = jnp.zeros((8, Y), F32)
        for p in range(4):
            for copy in last_down(p):
                copy.wait_recv()
            part = pl.ds(64 * p, 64)
            image = obuf[3, 0, part] + cbuf[3, 0, part] + cbuf[4, 0, part]
            light = obuf[3, 1, part] + cbuf[3, 1, part] + cbuf[4, 1, part]
            nbuf[pl.ds(64 * p + 8, 64)] = image / (1.0 + light)

            @pl.loop(2 * p, 2 * p + 2)
            def _(w):
                @pl.when(to_later)
                def _():
                    to_side(w, 0, me_t + 1).start()

                @pl.when(to_earlier)
                def _():
                    to_side(w, 5, me_t - 1).start()

            @pl.loop((0, 1, 3, 5)[p], (1, 3, 5, 8)[p])
            def _(w):
                @pl.when(w != me_w)
                def _():
                    to_strip(w).start()

        fbuf[1 + y] = nbuf[pl.ds(pl.multiple_of(me_w * STRIP, 8), STRIP + 16)]

    @pl.when(me_t == 0)
    def _():
        fbuf[0] = jnp.zeros((STRIP + 16, Y), F32)

    @pl.when(me_t == last)
    def _():
        fbuf[5] = jnp.zeros((STRIP + 16, Y), F32)

    for j in range(PLANES):

        @pl.when(jnp.logical_not(jnp.logical_and(c == 1, y == j)))
        def _():
            pltpu.make_async_copy(fbuf.at[1 + j], fbuf.at[1 + j], frecv.at[1 + j]).wait()

    @pl.when(me_t > 0)
    def _():
        pltpu.make_async_copy(fbuf.at[0, pl.ds(8, STRIP)], fbuf.at[0, pl.ds(8, STRIP)], frecv.at[0]).wait()

    @pl.when(me_t < last)
    def _():
        pltpu.make_async_copy(fbuf.at[5, pl.ds(8, STRIP)], fbuf.at[5, pl.ds(8, STRIP)], frecv.at[5]).wait()

    column = lax.broadcasted_iota(jnp.int32, (STRIP, Y), 1)
    for j in range(PLANES):
        center = fbuf[1 + j, pl.ds(8, STRIP)]
        beside = fbuf[j, pl.ds(8, STRIP)] + fbuf[2 + j, pl.ds(8, STRIP)]
        beside = beside + fbuf[1 + j, pl.ds(7, STRIP)] + fbuf[1 + j, pl.ds(9, STRIP)]
        before = jnp.where(column == 0, 0.0, pltpu.roll(center, 1, 1))
        after = jnp.where(column == Y - 1, 0.0, pltpu.roll(center, Y - 1, 1))
        out_ref[j] = beside + (before + after) - 6.0 * center

    for part, sem in ((head_out.at[pl.ds(0, 31), pl.ds(0, 136)], headsend), (sbuf.at[pl.ds(0, 93)], asend)):
        pltpu.make_async_copy(part, part, sem).wait()

    @pl.when(c == 0)
    def _():
        begin_up().wait_send()
        begin_down().wait_send()
        for q in range(1, 3):
            pass_down(q).wait_send()
        for p in range(4):
            for copy in last_down(p):
                copy.wait_send()

    @pl.when(c == 1)
    def _():
        for q in range(3):
            pass_up(q).wait_send()
        @pl.loop(1, NY * NC)
        def _(k):
            to_strip(lax.rem(me_w + k, NY * NC)).wait_send()

        @pl.loop(0, NY * NC)
        def _(w):
            @pl.when(to_later)
            def _():
                to_side(w, 0, me_t + 1).wait_send()

            @pl.when(to_earlier)
            def _():
                to_side(w, 5, me_t - 1).wait_send()


def per_device(source, receiver, corners):
    source = source.reshape(2, NX, NZ, PLANES, BX, BY)
    receiver = receiver.reshape(2, NX, NZ, PLANES, BX, BY)
    dma = pltpu.SemaphoreType.DMA
    return pl.pallas_call(
        kernel,
        out_shape=jax.ShapeDtypeStruct((PLANES, STRIP, Y), F32),
        in_specs=[
            pl.BlockSpec(memory_space=pltpu.HBM),
            pl.BlockSpec(memory_space=pltpu.HBM),
            pl.BlockSpec(memory_space=pltpu.HBM),
        ],
        out_specs=pl.BlockSpec(memory_space=pltpu.VMEM),
        scratch_shapes=[
            pltpu.SMEM((2, 2), jnp.int32),
            pltpu.VMEM((NZ, 2, 2, NX, NY, BX, BY), BF16),
            pltpu.VMEM((2 * NX * NY, 144, BY), BF16),
            pltpu.VMEM((6 * NX * NY, 128, BY), BF16),
            pltpu.VMEM((GROUP, 144, BY), BF16),
            pltpu.VMEM((3, GROUP, 128, BY), BF16),
            pltpu.VMEM((BLOCKS, X, 256), BF16),
            pltpu.VMEM((BLOCKS, 256, 128), BF16),
            pltpu.VMEM((4, 2, X, Y), F32),
            pltpu.VMEM((5, 2, X, Y), F32),
            pltpu.VMEM((X + 16, Y), F32),
            pltpu.VMEM((PLANES + 2, STRIP + 16, Y), F32),
            dma, dma((NZ, 2)), dma, dma, dma((4, BLOCKS)),
            dma((12,)), dma((12,)), dma((8,)), dma((8,)), dma((6,)),
        ],
        compiler_params=pltpu.CompilerParams(
            collective_id=0, has_side_effects=True, vmem_limit_bytes=67043328
        ),
        name="stack_shots",
    )(corners, source, receiver)


def solution(mesh):
    return jax.shard_map(
        per_device,
        mesh=mesh,
        in_specs=(
            P(("shot", "tile"), None, None, None, None),
            P(("shot", "tile"), None, None, None, None),
            P(("shot", "tile"), None),
        ),
        out_specs=P("tile", "shot", None),
        check_vma=False,
    )
```

```python
import functools

import jax
import jax.numpy as jnp
from jax import lax
from jax.experimental import pallas as pl
from jax.experimental.pallas import tpu as pltpu
from jax.sharding import PartitionSpec as P

MESH = pl.DeviceIdType.MESH
NX, NY, NZ, NC = 4, 4, 8, 2
GROUP = NX * NY * NC
BLOCKS = GROUP // 4
PLANES = NY
X = 256
Y = 256
BX = 32
BY = 128
STRIP = 32
F32 = jnp.float32
BF16 = jnp.bfloat16

ORDER = (
    (1, 0), (0, 1), (3, 3), (2, 1), (0, 3), (1, 2), (3, 0), (2, 2),
    (1, 1), (0, 2), (3, 1), (2, 3), (1, 3), (3, 2), (2, 0), (0, 0),
)


def kernel(
    corners_hbm, src_hbm, rcv_hbm, out_ref,
    corners_ref, lbuf, head_out, sbuf, head_in, rbuf, rows, mask, obuf, cbuf, nbuf, fbuf,
    cornersem, lsem, headsend, asend, arecv, bsend, brecv, nsend, hsend, frecv,
):
    me_w = lax.axis_index("shot")
    me_t = lax.axis_index("tile")
    y, c = me_w // NC, lax.rem(me_w, NC)
    x, z = me_t // NZ, lax.rem(me_t, NZ)
    me_g = x * (NY * NC) + me_w
    me_slot = 2 * (NX * NY - 1) + c
    up, down = lax.rem(z + 1, NZ), lax.rem(z + NZ - 1, NZ)

    def chip(dx, dy):
        return lax.rem(x + dx, NX), lax.rem(y + dy, NY)

    def remote(src, dst, send, recv, w, t):
        return pltpu.make_async_remote_copy(
            src_ref=src, dst_ref=dst, send_sem=send, recv_sem=recv,
            device_id=(w, t), device_id_type=MESH,
        )

    def depth_of(k):
        half = k // 2
        step = jnp.where(lax.rem(k, 2) == 0, half + 4, 3 - half)
        return lax.rem(z + step, NZ)

    def load(k):
        zt = depth_of(k)
        return (
            pltpu.make_async_copy(src_hbm.at[:, :, zt], lbuf.at[k, 0], lsem.at[k, 0]),
            pltpu.make_async_copy(rcv_hbm.at[:, :, zt], lbuf.at[k, 1], lsem.at[k, 1]),
        )

    corners_copy = pltpu.make_async_copy(corners_hbm, corners_ref, cornersem)
    corners_copy.start()
    for k in range(2):
        for copy in load(k):
            copy.start()

    barrier = pltpu.get_barrier_semaphore()

    def greet(w, t):
        pl.semaphore_signal(barrier, inc=1, device_id=(w, t), device_id_type=MESH)

    @pl.loop(1, GROUP)
    def _(g):
        other = lax.rem(me_g + g, GROUP)
        greet(lax.rem(other, NY * NC), (other // (NY * NC)) * NZ + z)

    for k in range(NC):
        greet(y * NC + k, x * NZ + up)
        greet(y * NC + k, x * NZ + down)
    last = NX * NZ - 1

    @pl.loop(0, NY * NC)
    def _(w):
        @pl.when(me_t > 0)
        def _():
            greet(w, me_t - 1)

        @pl.when(me_t < last)
        def _():
            greet(w, me_t + 1)

    @pl.loop(2, NZ)
    def _(k):
        for copy in load(k):
            copy.start()

    corners_copy.wait()
    first_col = [corners_ref[k, 1] for k in range(2)]
    lane = lax.broadcasted_iota(jnp.int32, (8, 128), 1)
    a = lax.rem(lane, BX)
    note = jnp.where(
        lane < 32,
        corners_ref[0, 0] + a,
        jnp.where(
            lane < 64,
            corners_ref[1, 0] + a,
            jnp.where(lane < 96, first_col[0] + 0 * lane, first_col[1] + 0 * lane),
        ),
    )
    note = note.astype(F32).astype(BF16)

    def turn(k, out, at):
        for copy in load(k):
            copy.wait()
        for which in range(2):
            for shot in range(2):
                block = lbuf[k, which, shot].reshape(NX * NY * BX, BY).astype(F32)
                block = pltpu.roll(block, lax.rem(first_col[shot], BY), 1).astype(BF16)
                out[pl.ds(at, 16), pl.ds(64 * which + 32 * shot, BX)] = block.reshape(NX * NY, BX, BY)

    def send(k, out, into, sem, q):
        core = lax.rem(k, 2)
        for p, (dx, dy) in enumerate(ORDER):
            tx, ty = chip(dx, dy)
            copy = remote(
                out(tx * NY + ty), into(2 * p + c), sem, arecv.at[q, p // 2],
                ty * NC + core, tx * NZ + z,
            )
            if (dx, dy) == (0, 0):
                pl.when(core != c)(copy.start)
            else:
                copy.start()

    def turn_head(k):
        turn(k, head_out, 16 * k)
        for h in range(16):
            head_out[16 * k + h, pl.ds(128, 8)] = note

        @pl.when(c == k)
        def _():
            head_in[me_slot, pl.ds(0, 136)] = head_out[16 * k + x * NY + y, pl.ds(0, 136)]

    def send_head(k):
        send(
            k,
            lambda chip: head_out.at[16 * k + chip, pl.ds(0, 136)],
            lambda slot: head_in.at[slot, pl.ds(0, 136)],
            headsend,
            0,
        )

    turn_head(0)
    edges = (me_t > 0).astype(jnp.int32) + (me_t < last).astype(jnp.int32)
    pl.semaphore_wait(barrier, GROUP - 1 + 2 * NC + NY * NC * edges)
    send_head(0)
    turn_head(1)
    send_head(1)

    @pl.loop(2, NZ)
    def _(k):
        q = k // 2
        at = (k - 2) * 16
        turn(k, sbuf, at)
        send(k, lambda chip: sbuf.at[at + chip], lambda slot: rbuf.at[q - 1, slot], asend, q)

        @pl.when(lax.rem(k, 2) == c)
        def _():
            rbuf[q - 1, me_slot] = sbuf[at + x * NY + y]

    def tables(i):
        row = lax.broadcasted_iota(jnp.int32, (X, 128), 0)
        wide = lax.broadcasted_iota(jnp.int32, (BX, 128), 1)
        first = wide[0:1]
        notes = [head_in[4 * i + s, pl.ds(128, 8)].astype(F32)[0:1].astype(jnp.int32) for s in range(4)]
        for h in range(2):
            both = jnp.where(first < 64, notes[2 * h], pltpu.roll(notes[2 * h + 1], 64, 1))
            rows[i, :, pl.ds(h * 128, 128)] = (row == both).astype(F32).astype(BF16)
        for s in range(4):
            for shot in range(2):
                col = notes[s][:, 64 + 32 * shot : 65 + 32 * shot]
                left = (wide >= col).astype(F32).astype(BF16)
                mask[i, pl.ds((2 * s + shot) * BX, BX), :] = left

    def place(q):
        def arrive(i, count):
            if q == 0:
                part = head_in.at[pl.ds(0, count), pl.ds(0, 136)]
            else:
                part = rbuf.at[q - 1, pl.ds(0, count)]
            pltpu.make_async_copy(part, part, arecv.at[q, i]).wait()

        def step(i, fresh):
            if q == 0:
                tables(i)
            got = head_in[pl.ds(4 * i, 4)] if q == 0 else rbuf[q - 1, pl.ds(4 * i, 4)]
            wave = got[:, 0:64].reshape(256, BY).astype(F32)
            back = got[:, 64:128].reshape(256, BY).astype(F32)
            keep = mask[i]
            table = rows[i]
            for which, value in ((0, wave * back), (1, wave * wave)):
                hi = value.astype(BF16)
                lo = (value - hi.astype(F32)).astype(BF16)
                hi_left, lo_left = hi * keep, lo * keep
                hi_both = jnp.concatenate((hi_left, hi - hi_left), axis=1)
                lo_both = jnp.concatenate((lo_left, lo - lo_left), axis=1)
                part = jnp.dot(table, hi_both, preferred_element_type=F32)
                part = part + jnp.dot(table, lo_both, preferred_element_type=F32)
                if fresh:
                    obuf[q, which] = part
                else:
                    obuf[q, which] += part

        arrive(0, 4)
        step(0, True)

        @pl.loop(1, BLOCKS - 1)
        def _(i):
            arrive(i, 4)
            step(i, False)

        arrive(BLOCKS - 1, 3)
        step(BLOCKS - 1, False)

    def begin_up():
        return remote(obuf.at[0, 0], cbuf.at[0, 0], bsend.at[0], brecv.at[0], y * NC + 1, x * NZ + up)

    def begin_down():
        return remote(obuf.at[0, 1], cbuf.at[1, 1], bsend.at[1], brecv.at[1], y * NC, x * NZ + down)

    def pass_down(q):
        return remote(obuf.at[q], cbuf.at[q + 1], bsend.at[q + 1], brecv.at[q + 1], y * NC, x * NZ + down)

    def last_down(p):
        part = pl.ds(64 * p, 64)
        return tuple(
            remote(
                obuf.at[3, h, part], cbuf.at[4, h, part], bsend.at[4 + 2 * p + h], brecv.at[4 + 2 * p + h],
                y * NC + 1, x * NZ + down,
            )
            for h in range(2)
        )

    def pass_up(q):
        return remote(obuf.at[q], cbuf.at[q + 1], bsend.at[q + 1], brecv.at[q + 1], y * NC + 1, x * NZ + up)

    for q in range(4):
        place(q)

        @pl.when(c == 0)
        def _():
            if q == 0:
                begin_up().start()
                begin_down().start()
            elif q == 1:
                begin_down().wait_recv()
                obuf[1, 1] += cbuf[1, 1]
                pass_down(1).start()
            else:
                pass_down(q - 1).wait_recv()
                if q < 3:
                    obuf[q] += cbuf[q]
                    pass_down(q).start()
                else:
                    for p in range(4):
                        part = pl.ds(64 * p, 64)
                        obuf[3, :, part] += cbuf[3, :, part]
                        for copy in last_down(p):
                            copy.start()

        @pl.when(c == 1)
        def _():
            if q == 0:
                begin_up().wait_recv()
                obuf[0, 0] += cbuf[0, 0]
                pass_up(0).start()
            elif q < 3:
                pass_up(q - 1).wait_recv()
                obuf[q] += cbuf[q]
                pass_up(q).start()
            else:
                pass_up(2).wait_recv()

    def to_strip(w):
        return remote(
            nbuf.at[pl.ds(pl.multiple_of(w * STRIP, 8), STRIP + 16)], fbuf.at[1 + y],
            nsend.at[w], frecv.at[1 + y], w, me_t,
        )

    def to_side(w, plane, t):
        return remote(
            nbuf.at[pl.ds(pl.multiple_of(w * STRIP + 8, 8), STRIP)], fbuf.at[plane, pl.ds(8, STRIP)],
            hsend.at[w], frecv.at[plane], w, t,
        )

    to_later = jnp.logical_and(y == NY - 1, me_t < last)
    to_earlier = jnp.logical_and(y == 0, me_t > 0)

    @pl.when(c == 1)
    def _():
        nbuf[pl.ds(0, 8)] = jnp.zeros((8, Y), F32)
        nbuf[pl.ds(X + 8, 8)] = jnp.zeros((8, Y), F32)
        for p in range(4):
            for copy in last_down(p):
                copy.wait_recv()
            part = pl.ds(64 * p, 64)
            image = obuf[3, 0, part] + cbuf[3, 0, part] + cbuf[4, 0, part]
            light = obuf[3, 1, part] + cbuf[3, 1, part] + cbuf[4, 1, part]
            nbuf[pl.ds(64 * p + 8, 64)] = image / (1.0 + light)

            @pl.loop(2 * p, 2 * p + 2)
            def _(w):
                @pl.when(to_later)
                def _():
                    to_side(w, 0, me_t + 1).start()

                @pl.when(to_earlier)
                def _():
                    to_side(w, 5, me_t - 1).start()

            @pl.loop((0, 1, 3, 5)[p], (1, 3, 5, 8)[p])
            def _(w):
                @pl.when(w != me_w)
                def _():
                    to_strip(w).start()

        fbuf[1 + y] = nbuf[pl.ds(pl.multiple_of(me_w * STRIP, 8), STRIP + 16)]

    @pl.when(me_t == 0)
    def _():
        fbuf[0] = jnp.zeros((STRIP + 16, Y), F32)

    @pl.when(me_t == last)
    def _():
        fbuf[5] = jnp.zeros((STRIP + 16, Y), F32)

    for j in range(PLANES):

        @pl.when(jnp.logical_not(jnp.logical_and(c == 1, y == j)))
        def _():
            pltpu.make_async_copy(fbuf.at[1 + j], fbuf.at[1 + j], frecv.at[1 + j]).wait()

    @pl.when(me_t > 0)
    def _():
        pltpu.make_async_copy(fbuf.at[0, pl.ds(8, STRIP)], fbuf.at[0, pl.ds(8, STRIP)], frecv.at[0]).wait()

    @pl.when(me_t < last)
    def _():
        pltpu.make_async_copy(fbuf.at[5, pl.ds(8, STRIP)], fbuf.at[5, pl.ds(8, STRIP)], frecv.at[5]).wait()

    column = lax.broadcasted_iota(jnp.int32, (STRIP, Y), 1)
    for j in range(PLANES):
        center = fbuf[1 + j, pl.ds(8, STRIP)]
        beside = fbuf[j, pl.ds(8, STRIP)] + fbuf[2 + j, pl.ds(8, STRIP)]
        beside = beside + fbuf[1 + j, pl.ds(7, STRIP)] + fbuf[1 + j, pl.ds(9, STRIP)]
        before = jnp.where(column == 0, 0.0, pltpu.roll(center, 1, 1))
        after = jnp.where(column == Y - 1, 0.0, pltpu.roll(center, Y - 1, 1))
        out_ref[j] = beside + (before + after) - 6.0 * center

    for part, sem in ((head_out.at[pl.ds(0, 31), pl.ds(0, 136)], headsend), (sbuf.at[pl.ds(0, 93)], asend)):
        pltpu.make_async_copy(part, part, sem).wait()

    @pl.when(c == 0)
    def _():
        begin_up().wait_send()
        begin_down().wait_send()
        for q in range(1, 3):
            pass_down(q).wait_send()
        for p in range(4):
            for copy in last_down(p):
                copy.wait_send()

    @pl.when(c == 1)
    def _():
        for q in range(3):
            pass_up(q).wait_send()
        @pl.loop(1, NY * NC)
        def _(k):
            to_strip(lax.rem(me_w + k, NY * NC)).wait_send()

        @pl.loop(0, NY * NC)
        def _(w):
            @pl.when(to_later)
            def _():
                to_side(w, 0, me_t + 1).wait_send()

            @pl.when(to_earlier)
            def _():
                to_side(w, 5, me_t - 1).wait_send()


def per_device(source, receiver, corners):
    source = source.reshape(2, NX, NZ, PLANES, BX, BY)
    receiver = receiver.reshape(2, NX, NZ, PLANES, BX, BY)
    dma = pltpu.SemaphoreType.DMA
    return pl.pallas_call(
        kernel,
        out_shape=jax.ShapeDtypeStruct((PLANES, STRIP, Y), F32),
        in_specs=[
            pl.BlockSpec(memory_space=pltpu.HBM),
            pl.BlockSpec(memory_space=pltpu.HBM),
            pl.BlockSpec(memory_space=pltpu.HBM),
        ],
        out_specs=pl.BlockSpec(memory_space=pltpu.VMEM),
        scratch_shapes=[
            pltpu.SMEM((2, 2), jnp.int32),
            pltpu.VMEM((NZ, 2, 2, NX, NY, BX, BY), BF16),
            pltpu.VMEM((2 * NX * NY, 144, BY), BF16),
            pltpu.VMEM((6 * NX * NY, 128, BY), BF16),
            pltpu.VMEM((GROUP, 144, BY), BF16),
            pltpu.VMEM((3, GROUP, 128, BY), BF16),
            pltpu.VMEM((BLOCKS, X, 256), BF16),
            pltpu.VMEM((BLOCKS, 256, 128), BF16),
            pltpu.VMEM((4, 2, X, Y), F32),
            pltpu.VMEM((5, 2, X, Y), F32),
            pltpu.VMEM((X + 16, Y), F32),
            pltpu.VMEM((PLANES + 2, STRIP + 16, Y), F32),
            dma, dma((NZ, 2)), dma, dma, dma((4, BLOCKS)),
            dma((12,)), dma((12,)), dma((8,)), dma((8,)), dma((6,)),
        ],
        compiler_params=pltpu.CompilerParams(
            collective_id=0, has_side_effects=True, vmem_limit_bytes=56000000
        ),
        name="stack_shots",
    )(corners, source, receiver)


def solution(mesh):
    return jax.shard_map(
        per_device,
        mesh=mesh,
        in_specs=(
            P(("shot", "tile"), None, None, None, None),
            P(("shot", "tile"), None, None, None, None),
            P(("shot", "tile"), None),
        ),
        out_specs=P("tile", "shot", None),
        check_vma=False,
    )
```

```python
import functools

import jax
import jax.numpy as jnp
from jax import lax
from jax.experimental import pallas as pl
from jax.experimental.pallas import tpu as pltpu
from jax.sharding import PartitionSpec as P

MESH = pl.DeviceIdType.MESH
NX, NY, NZ, NC = 4, 4, 8, 2
GROUP = NX * NY * NC
BLOCKS = GROUP // 4
PLANES = NY
X = 256
Y = 256
BX = 32
BY = 128
STRIP = 32
F32 = jnp.float32
BF16 = jnp.bfloat16

ORDER = (
    (0, 3), (3, 0), (0, 1), (1, 0), (0, 2), (1, 3), (2, 0), (3, 1),
    (1, 1), (3, 3), (2, 1), (2, 3), (1, 2), (3, 2), (2, 2), (0, 0),
)


def kernel(
    corners_hbm, src_hbm, rcv_hbm, out_ref,
    corners_ref, lbuf, head_out, sbuf, head_in, rbuf, rows, mask, obuf, cbuf, nbuf, fbuf,
    cornersem, lsem, headsend, asend, arecv, bsend, brecv, nsend, hsend, frecv,
):
    me_w = lax.axis_index("shot")
    me_t = lax.axis_index("tile")
    y, c = me_w // NC, lax.rem(me_w, NC)
    x, z = me_t // NZ, lax.rem(me_t, NZ)
    me_g = x * (NY * NC) + me_w
    me_slot = 2 * (NX * NY - 1) + c
    up, down = lax.rem(z + 1, NZ), lax.rem(z + NZ - 1, NZ)

    def chip(dx, dy):
        return lax.rem(x + dx, NX), lax.rem(y + dy, NY)

    def remote(src, dst, send, recv, w, t):
        return pltpu.make_async_remote_copy(
            src_ref=src, dst_ref=dst, send_sem=send, recv_sem=recv,
            device_id=(w, t), device_id_type=MESH,
        )

    def depth_of(k):
        half = k // 2
        step = jnp.where(lax.rem(k, 2) == 0, half + 4, 3 - half)
        return lax.rem(z + step, NZ)

    def load(k):
        zt = depth_of(k)
        return (
            pltpu.make_async_copy(src_hbm.at[:, :, zt], lbuf.at[k, 0], lsem.at[k, 0]),
            pltpu.make_async_copy(rcv_hbm.at[:, :, zt], lbuf.at[k, 1], lsem.at[k, 1]),
        )

    corners_copy = pltpu.make_async_copy(corners_hbm, corners_ref, cornersem)
    corners_copy.start()
    for k in range(2):
        for copy in load(k):
            copy.start()

    barrier = pltpu.get_barrier_semaphore()

    def greet(w, t):
        pl.semaphore_signal(barrier, inc=1, device_id=(w, t), device_id_type=MESH)

    @pl.loop(1, GROUP)
    def _(g):
        other = lax.rem(me_g + g, GROUP)
        greet(lax.rem(other, NY * NC), (other // (NY * NC)) * NZ + z)

    for k in range(NC):
        greet(y * NC + k, x * NZ + up)
        greet(y * NC + k, x * NZ + down)
    last = NX * NZ - 1

    @pl.loop(0, NY * NC)
    def _(w):
        @pl.when(me_t > 0)
        def _():
            greet(w, me_t - 1)

        @pl.when(me_t < last)
        def _():
            greet(w, me_t + 1)

    @pl.loop(2, NZ)
    def _(k):
        for copy in load(k):
            copy.start()

    corners_copy.wait()
    first_col = [corners_ref[k, 1] for k in range(2)]
    lane = lax.broadcasted_iota(jnp.int32, (8, 128), 1)
    a = lax.rem(lane, BX)
    note = jnp.where(
        lane < 32,
        corners_ref[0, 0] + a,
        jnp.where(
            lane < 64,
            corners_ref[1, 0] + a,
            jnp.where(lane < 96, first_col[0] + 0 * lane, first_col[1] + 0 * lane),
        ),
    )
    note = note.astype(F32).astype(BF16)

    def turn(k, out, at):
        for copy in load(k):
            copy.wait()
        for which in range(2):
            for shot in range(2):
                block = lbuf[k, which, shot].reshape(NX * NY * BX, BY).astype(F32)
                block = pltpu.roll(block, lax.rem(first_col[shot], BY), 1).astype(BF16)
                out[pl.ds(at, 16), pl.ds(64 * which + 32 * shot, BX)] = block.reshape(NX * NY, BX, BY)

    def send(k, out, into, sem, q):
        core = lax.rem(k, 2)
        for p, (dx, dy) in enumerate(ORDER):
            tx, ty = chip(dx, dy)
            copy = remote(
                out(tx * NY + ty), into(2 * p + c), sem, arecv.at[q, p // 2],
                ty * NC + core, tx * NZ + z,
            )
            if (dx, dy) == (0, 0):
                pl.when(core != c)(copy.start)
            else:
                copy.start()

    def turn_head(k):
        turn(k, head_out, 16 * k)
        for h in range(16):
            head_out[16 * k + h, pl.ds(128, 8)] = note

        @pl.when(c == k)
        def _():
            head_in[me_slot, pl.ds(0, 136)] = head_out[16 * k + x * NY + y, pl.ds(0, 136)]

    def send_head(k):
        send(
            k,
            lambda chip: head_out.at[16 * k + chip, pl.ds(0, 136)],
            lambda slot: head_in.at[slot, pl.ds(0, 136)],
            headsend,
            0,
        )

    turn_head(0)
    edges = (me_t > 0).astype(jnp.int32) + (me_t < last).astype(jnp.int32)
    pl.semaphore_wait(barrier, GROUP - 1 + 2 * NC + NY * NC * edges)
    send_head(0)
    turn_head(1)
    send_head(1)

    @pl.loop(2, NZ)
    def _(k):
        q = k // 2
        at = (k - 2) * 16
        turn(k, sbuf, at)
        send(k, lambda chip: sbuf.at[at + chip], lambda slot: rbuf.at[q - 1, slot], asend, q)

        @pl.when(lax.rem(k, 2) == c)
        def _():
            rbuf[q - 1, me_slot] = sbuf[at + x * NY + y]

    def tables(i):
        row = lax.broadcasted_iota(jnp.int32, (X, 128), 0)
        wide = lax.broadcasted_iota(jnp.int32, (BX, 128), 1)
        first = wide[0:1]
        notes = [head_in[4 * i + s, pl.ds(128, 8)].astype(F32)[0:1].astype(jnp.int32) for s in range(4)]
        for h in range(2):
            both = jnp.where(first < 64, notes[2 * h], pltpu.roll(notes[2 * h + 1], 64, 1))
            rows[i, :, pl.ds(h * 128, 128)] = (row == both).astype(F32).astype(BF16)
        for s in range(4):
            for shot in range(2):
                col = notes[s][:, 64 + 32 * shot : 65 + 32 * shot]
                left = (wide >= col).astype(F32).astype(BF16)
                mask[i, pl.ds((2 * s + shot) * BX, BX), :] = left

    def place(q):
        def arrive(i, count):
            if q == 0:
                part = head_in.at[pl.ds(0, count), pl.ds(0, 136)]
            else:
                part = rbuf.at[q - 1, pl.ds(0, count)]
            pltpu.make_async_copy(part, part, arecv.at[q, i]).wait()

        def step(i, fresh):
            if q == 0:
                tables(i)
            got = head_in[pl.ds(4 * i, 4)] if q == 0 else rbuf[q - 1, pl.ds(4 * i, 4)]
            wave = got[:, 0:64].reshape(256, BY).astype(F32)
            back = got[:, 64:128].reshape(256, BY).astype(F32)
            keep = mask[i]
            table = rows[i]
            for which, value in ((0, wave * back), (1, wave * wave)):
                hi = value.astype(BF16)
                lo = (value - hi.astype(F32)).astype(BF16)
                hi_left, lo_left = hi * keep, lo * keep
                hi_both = jnp.concatenate((hi_left, hi - hi_left), axis=1)
                lo_both = jnp.concatenate((lo_left, lo - lo_left), axis=1)
                part = jnp.dot(table, hi_both, preferred_element_type=F32)
                part = part + jnp.dot(table, lo_both, preferred_element_type=F32)
                if fresh:
                    obuf[q, which] = part
                else:
                    obuf[q, which] += part

        arrive(0, 4)
        step(0, True)

        @pl.loop(1, BLOCKS - 1)
        def _(i):
            arrive(i, 4)
            step(i, False)

        arrive(BLOCKS - 1, 3)
        step(BLOCKS - 1, False)

    def begin_up():
        return remote(obuf.at[0, 0], cbuf.at[0, 0], bsend.at[0], brecv.at[0], y * NC + 1, x * NZ + up)

    def begin_down():
        return remote(obuf.at[0, 1], cbuf.at[1, 1], bsend.at[1], brecv.at[1], y * NC, x * NZ + down)

    def pass_down(q):
        return remote(obuf.at[q], cbuf.at[q + 1], bsend.at[q + 1], brecv.at[q + 1], y * NC, x * NZ + down)

    def last_down(p):
        part = pl.ds(64 * p, 64)
        return tuple(
            remote(
                obuf.at[3, h, part], cbuf.at[4, h, part], bsend.at[4 + 2 * p + h], brecv.at[4 + 2 * p + h],
                y * NC + 1, x * NZ + down,
            )
            for h in range(2)
        )

    def pass_up(q):
        return remote(obuf.at[q], cbuf.at[q + 1], bsend.at[q + 1], brecv.at[q + 1], y * NC + 1, x * NZ + up)

    for q in range(4):
        place(q)

        @pl.when(c == 0)
        def _():
            if q == 0:
                begin_up().start()
                begin_down().start()
            elif q == 1:
                begin_down().wait_recv()
                obuf[1, 1] += cbuf[1, 1]
                pass_down(1).start()
            else:
                pass_down(q - 1).wait_recv()
                if q < 3:
                    obuf[q] += cbuf[q]
                    pass_down(q).start()
                else:
                    for p in range(4):
                        part = pl.ds(64 * p, 64)
                        obuf[3, :, part] += cbuf[3, :, part]
                        for copy in last_down(p):
                            copy.start()

        @pl.when(c == 1)
        def _():
            if q == 0:
                begin_up().wait_recv()
                obuf[0, 0] += cbuf[0, 0]
                pass_up(0).start()
            elif q < 3:
                pass_up(q - 1).wait_recv()
                obuf[q] += cbuf[q]
                pass_up(q).start()
            else:
                pass_up(2).wait_recv()

    def to_strip(w):
        return remote(
            nbuf.at[pl.ds(pl.multiple_of(w * STRIP, 8), STRIP + 16)], fbuf.at[1 + y],
            nsend.at[w], frecv.at[1 + y], w, me_t,
        )

    def to_side(w, plane, t):
        return remote(
            nbuf.at[pl.ds(pl.multiple_of(w * STRIP + 8, 8), STRIP)], fbuf.at[plane, pl.ds(8, STRIP)],
            hsend.at[w], frecv.at[plane], w, t,
        )

    to_later = jnp.logical_and(y == NY - 1, me_t < last)
    to_earlier = jnp.logical_and(y == 0, me_t > 0)

    @pl.when(c == 1)
    def _():
        nbuf[pl.ds(0, 8)] = jnp.zeros((8, Y), F32)
        nbuf[pl.ds(X + 8, 8)] = jnp.zeros((8, Y), F32)
        for p in range(4):
            for copy in last_down(p):
                copy.wait_recv()
            part = pl.ds(64 * p, 64)
            image = obuf[3, 0, part] + cbuf[3, 0, part] + cbuf[4, 0, part]
            light = obuf[3, 1, part] + cbuf[3, 1, part] + cbuf[4, 1, part]
            nbuf[pl.ds(64 * p + 8, 64)] = image / (1.0 + light)

            @pl.loop(2 * p, 2 * p + 2)
            def _(w):
                @pl.when(to_later)
                def _():
                    to_side(w, 0, me_t + 1).start()

                @pl.when(to_earlier)
                def _():
                    to_side(w, 5, me_t - 1).start()

            @pl.loop((0, 1, 3, 5)[p], (1, 3, 5, 8)[p])
            def _(w):
                @pl.when(w != me_w)
                def _():
                    to_strip(w).start()

        fbuf[1 + y] = nbuf[pl.ds(pl.multiple_of(me_w * STRIP, 8), STRIP + 16)]

    @pl.when(me_t == 0)
    def _():
        fbuf[0] = jnp.zeros((STRIP + 16, Y), F32)

    @pl.when(me_t == last)
    def _():
        fbuf[5] = jnp.zeros((STRIP + 16, Y), F32)

    for j in range(PLANES):

        @pl.when(jnp.logical_not(jnp.logical_and(c == 1, y == j)))
        def _():
            pltpu.make_async_copy(fbuf.at[1 + j], fbuf.at[1 + j], frecv.at[1 + j]).wait()

    @pl.when(me_t > 0)
    def _():
        pltpu.make_async_copy(fbuf.at[0, pl.ds(8, STRIP)], fbuf.at[0, pl.ds(8, STRIP)], frecv.at[0]).wait()

    @pl.when(me_t < last)
    def _():
        pltpu.make_async_copy(fbuf.at[5, pl.ds(8, STRIP)], fbuf.at[5, pl.ds(8, STRIP)], frecv.at[5]).wait()

    column = lax.broadcasted_iota(jnp.int32, (STRIP, Y), 1)
    for j in range(PLANES):
        center = fbuf[1 + j, pl.ds(8, STRIP)]
        beside = fbuf[j, pl.ds(8, STRIP)] + fbuf[2 + j, pl.ds(8, STRIP)]
        beside = beside + fbuf[1 + j, pl.ds(7, STRIP)] + fbuf[1 + j, pl.ds(9, STRIP)]
        before = jnp.where(column == 0, 0.0, pltpu.roll(center, 1, 1))
        after = jnp.where(column == Y - 1, 0.0, pltpu.roll(center, Y - 1, 1))
        out_ref[j] = beside + (before + after) - 6.0 * center

    for part, sem in ((head_out.at[pl.ds(0, 31), pl.ds(0, 136)], headsend), (sbuf.at[pl.ds(0, 93)], asend)):
        pltpu.make_async_copy(part, part, sem).wait()

    @pl.when(c == 0)
    def _():
        begin_up().wait_send()
        begin_down().wait_send()
        for q in range(1, 3):
            pass_down(q).wait_send()
        for p in range(4):
            for copy in last_down(p):
                copy.wait_send()

    @pl.when(c == 1)
    def _():
        for q in range(3):
            pass_up(q).wait_send()
        @pl.loop(1, NY * NC)
        def _(k):
            to_strip(lax.rem(me_w + k, NY * NC)).wait_send()

        @pl.loop(0, NY * NC)
        def _(w):
            @pl.when(to_later)
            def _():
                to_side(w, 0, me_t + 1).wait_send()

            @pl.when(to_earlier)
            def _():
                to_side(w, 5, me_t - 1).wait_send()


def per_device(source, receiver, corners):
    source = source.reshape(2, NX, NZ, PLANES, BX, BY)
    receiver = receiver.reshape(2, NX, NZ, PLANES, BX, BY)
    dma = pltpu.SemaphoreType.DMA
    return pl.pallas_call(
        kernel,
        out_shape=jax.ShapeDtypeStruct((PLANES, STRIP, Y), F32),
        in_specs=[
            pl.BlockSpec(memory_space=pltpu.HBM),
            pl.BlockSpec(memory_space=pltpu.HBM),
            pl.BlockSpec(memory_space=pltpu.HBM),
        ],
        out_specs=pl.BlockSpec(memory_space=pltpu.VMEM),
        scratch_shapes=[
            pltpu.SMEM((2, 2), jnp.int32),
            pltpu.VMEM((NZ, 2, 2, NX, NY, BX, BY), BF16),
            pltpu.VMEM((2 * NX * NY, 144, BY), BF16),
            pltpu.VMEM((6 * NX * NY, 128, BY), BF16),
            pltpu.VMEM((GROUP, 144, BY), BF16),
            pltpu.VMEM((3, GROUP, 128, BY), BF16),
            pltpu.VMEM((BLOCKS, X, 256), BF16),
            pltpu.VMEM((BLOCKS, 256, 128), BF16),
            pltpu.VMEM((4, 2, X, Y), F32),
            pltpu.VMEM((5, 2, X, Y), F32),
            pltpu.VMEM((X + 16, Y), F32),
            pltpu.VMEM((PLANES + 2, STRIP + 16, Y), F32),
            dma, dma((NZ, 2)), dma, dma, dma((4, BLOCKS)),
            dma((12,)), dma((12,)), dma((8,)), dma((8,)), dma((6,)),
        ],
        compiler_params=pltpu.CompilerParams(
            collective_id=0, has_side_effects=True, vmem_limit_bytes=56_000_000
        ),
        name="stack_shots",
    )(corners, source, receiver)


def solution(mesh):
    return jax.shard_map(
        per_device,
        mesh=mesh,
        in_specs=(
            P(("shot", "tile"), None, None, None, None),
            P(("shot", "tile"), None, None, None, None),
            P(("shot", "tile"), None),
        ),
        out_specs=P("tile", "shot", None),
        check_vma=False,
    )
```

```python
import functools

import jax
import jax.numpy as jnp
from jax import lax
from jax.experimental import pallas as pl
from jax.experimental.pallas import tpu as pltpu
from jax.sharding import PartitionSpec as P

MESH = pl.DeviceIdType.MESH
NX, NY, NZ, NC = 4, 4, 8, 2
GROUP = NX * NY * NC
BLOCKS = GROUP // 4
PLANES = NY
X = 256
Y = 256
BX = 32
BY = 128
STRIP = 32
F32 = jnp.float32
BF16 = jnp.bfloat16

ORDER = (
    (0, 3), (3, 0), (0, 1), (1, 0), (0, 2), (1, 3), (2, 0), (3, 1),
    (1, 1), (3, 3), (2, 1), (2, 3), (1, 2), (3, 2), (2, 2), (0, 0),
)


def kernel(
    corners_hbm, src_hbm, rcv_hbm, out_ref,
    corners_ref, lbuf, head_out, sbuf, head_in, rbuf, rows, mask, obuf, cbuf, nbuf, fbuf,
    cornersem, lsem, headsend, asend, arecv, bsend, brecv, nsend, hsend, frecv,
):
    me_w = lax.axis_index("shot")
    me_t = lax.axis_index("tile")
    y, c = me_w // NC, lax.rem(me_w, NC)
    x, z = me_t // NZ, lax.rem(me_t, NZ)
    me_g = x * (NY * NC) + me_w
    me_slot = 2 * (NX * NY - 1) + c
    up, down = lax.rem(z + 1, NZ), lax.rem(z + NZ - 1, NZ)

    def chip(dx, dy):
        return lax.rem(x + dx, NX), lax.rem(y + dy, NY)

    def remote(src, dst, send, recv, w, t):
        return pltpu.make_async_remote_copy(
            src_ref=src, dst_ref=dst, send_sem=send, recv_sem=recv,
            device_id=(w, t), device_id_type=MESH,
        )

    def depth_of(k):
        half = k // 2
        step = jnp.where(lax.rem(k, 2) == 0, half + 4, 3 - half)
        return lax.rem(z + step, NZ)

    def load(k):
        zt = depth_of(k)
        return (
            pltpu.make_async_copy(src_hbm.at[:, :, zt], lbuf.at[k, 0], lsem.at[k, 0]),
            pltpu.make_async_copy(rcv_hbm.at[:, :, zt], lbuf.at[k, 1], lsem.at[k, 1]),
        )

    corners_copy = pltpu.make_async_copy(corners_hbm, corners_ref, cornersem)
    corners_copy.start()
    for k in range(2):
        for copy in load(k):
            copy.start()

    barrier = pltpu.get_barrier_semaphore()

    def greet(w, t):
        pl.semaphore_signal(barrier, inc=1, device_id=(w, t), device_id_type=MESH)

    for dx, dy in ORDER[:-1]:
        tx, ty = chip(dx, dy)
        for k in range(NC):
            greet(ty * NC + k, tx * NZ + z)
    greet(y * NC + 1 - c, me_t)

    for k in range(NC):
        greet(y * NC + k, x * NZ + up)
        greet(y * NC + k, x * NZ + down)
    last = NX * NZ - 1

    @pl.loop(0, NY * NC)
    def _(w):
        @pl.when(me_t > 0)
        def _():
            greet(w, me_t - 1)

        @pl.when(me_t < last)
        def _():
            greet(w, me_t + 1)

    @pl.loop(2, NZ)
    def _(k):
        for copy in load(k):
            copy.start()

    corners_copy.wait()
    first_col = [corners_ref[k, 1] for k in range(2)]
    lane = lax.broadcasted_iota(jnp.int32, (8, 128), 1)
    a = lax.rem(lane, BX)
    note = jnp.where(
        lane < 32,
        corners_ref[0, 0] + a,
        jnp.where(
            lane < 64,
            corners_ref[1, 0] + a,
            jnp.where(lane < 96, first_col[0] + 0 * lane, first_col[1] + 0 * lane),
        ),
    )
    note = note.astype(F32).astype(BF16)

    def turn(k, out, at):
        for copy in load(k):
            copy.wait()
        for which in range(2):
            for shot in range(2):
                block = lbuf[k, which, shot].reshape(NX * NY * BX, BY).astype(F32)
                block = pltpu.roll(block, lax.rem(first_col[shot], BY), 1).astype(BF16)
                out[pl.ds(at, 16), pl.ds(64 * which + 32 * shot, BX)] = block.reshape(NX * NY, BX, BY)

    def send(k, out, into, sem, q):
        core = lax.rem(k, 2)
        for p, (dx, dy) in enumerate(ORDER):
            tx, ty = chip(dx, dy)
            copy = remote(
                out(tx * NY + ty), into(2 * p + c), sem, arecv.at[q, p // 2],
                ty * NC + core, tx * NZ + z,
            )
            if (dx, dy) == (0, 0):
                pl.when(core != c)(copy.start)
            else:
                copy.start()

    def turn_head(k):
        turn(k, head_out, 16 * k)
        for h in range(16):
            head_out[16 * k + h, pl.ds(128, 8)] = note

        @pl.when(c == k)
        def _():
            head_in[me_slot, pl.ds(0, 136)] = head_out[16 * k + x * NY + y, pl.ds(0, 136)]

    def send_head(k):
        send(
            k,
            lambda chip: head_out.at[16 * k + chip, pl.ds(0, 136)],
            lambda slot: head_in.at[slot, pl.ds(0, 136)],
            headsend,
            0,
        )

    turn_head(0)
    edges = (me_t > 0).astype(jnp.int32) + (me_t < last).astype(jnp.int32)
    pl.semaphore_wait(barrier, GROUP - 1 + 2 * NC + NY * NC * edges)
    send_head(0)
    turn_head(1)
    send_head(1)

    @pl.loop(2, NZ)
    def _(k):
        q = k // 2
        at = (k - 2) * 16
        turn(k, sbuf, at)
        send(k, lambda chip: sbuf.at[at + chip], lambda slot: rbuf.at[q - 1, slot], asend, q)

        @pl.when(lax.rem(k, 2) == c)
        def _():
            rbuf[q - 1, me_slot] = sbuf[at + x * NY + y]

    def tables(i):
        row = lax.broadcasted_iota(jnp.int32, (X, 128), 0)
        wide = lax.broadcasted_iota(jnp.int32, (BX, 128), 1)
        first = wide[0:1]
        notes = [head_in[4 * i + s, pl.ds(128, 8)].astype(F32)[0:1].astype(jnp.int32) for s in range(4)]
        for h in range(2):
            both = jnp.where(first < 64, notes[2 * h], pltpu.roll(notes[2 * h + 1], 64, 1))
            rows[i, :, pl.ds(h * 128, 128)] = (row == both).astype(F32).astype(BF16)
        for s in range(4):
            for shot in range(2):
                col = notes[s][:, 64 + 32 * shot : 65 + 32 * shot]
                left = (wide >= col).astype(F32).astype(BF16)
                mask[i, pl.ds((2 * s + shot) * BX, BX), :] = left

    def place(q):
        def arrive(i, count):
            if q == 0:
                part = head_in.at[pl.ds(0, count), pl.ds(0, 136)]
            else:
                part = rbuf.at[q - 1, pl.ds(0, count)]
            pltpu.make_async_copy(part, part, arecv.at[q, i]).wait()

        def step(i, fresh):
            if q == 0:
                tables(i)
            got = head_in[pl.ds(4 * i, 4)] if q == 0 else rbuf[q - 1, pl.ds(4 * i, 4)]
            wave = got[:, 0:64].reshape(256, BY).astype(F32)
            back = got[:, 64:128].reshape(256, BY).astype(F32)
            keep = mask[i]
            table = rows[i]
            for which, value in ((0, wave * back), (1, wave * wave)):
                hi = value.astype(BF16)
                lo = (value - hi.astype(F32)).astype(BF16)
                hi_left, lo_left = hi * keep, lo * keep
                hi_both = jnp.concatenate((hi_left, hi - hi_left), axis=1)
                lo_both = jnp.concatenate((lo_left, lo - lo_left), axis=1)
                part = jnp.dot(table, hi_both, preferred_element_type=F32)
                part = part + jnp.dot(table, lo_both, preferred_element_type=F32)
                if fresh:
                    obuf[q, which] = part
                else:
                    obuf[q, which] += part

        arrive(0, 4)
        step(0, True)

        @pl.loop(1, BLOCKS - 1)
        def _(i):
            arrive(i, 4)
            step(i, False)

        arrive(BLOCKS - 1, 3)
        step(BLOCKS - 1, False)

    def begin_up():
        return remote(obuf.at[0, 0], cbuf.at[0, 0], bsend.at[0], brecv.at[0], y * NC + 1, x * NZ + up)

    def begin_down():
        return remote(obuf.at[0, 1], cbuf.at[1, 1], bsend.at[1], brecv.at[1], y * NC, x * NZ + down)

    def pass_down(q):
        return remote(obuf.at[q], cbuf.at[q + 1], bsend.at[q + 1], brecv.at[q + 1], y * NC, x * NZ + down)

    def last_down(p):
        part = pl.ds(64 * p, 64)
        return tuple(
            remote(
                obuf.at[3, h, part], cbuf.at[4, h, part], bsend.at[4 + 2 * p + h], brecv.at[4 + 2 * p + h],
                y * NC + 1, x * NZ + down,
            )
            for h in range(2)
        )

    def pass_up(q):
        return remote(obuf.at[q], cbuf.at[q + 1], bsend.at[q + 1], brecv.at[q + 1], y * NC + 1, x * NZ + up)

    for q in range(4):
        place(q)

        @pl.when(c == 0)
        def _():
            if q == 0:
                begin_up().start()
                begin_down().start()
            elif q == 1:
                begin_down().wait_recv()
                obuf[1, 1] += cbuf[1, 1]
                pass_down(1).start()
            else:
                pass_down(q - 1).wait_recv()
                if q < 3:
                    obuf[q] += cbuf[q]
                    pass_down(q).start()
                else:
                    for p in range(4):
                        part = pl.ds(64 * p, 64)
                        obuf[3, :, part] += cbuf[3, :, part]
                        for copy in last_down(p):
                            copy.start()

        @pl.when(c == 1)
        def _():
            if q == 0:
                begin_up().wait_recv()
                obuf[0, 0] += cbuf[0, 0]
                pass_up(0).start()
            elif q < 3:
                pass_up(q - 1).wait_recv()
                obuf[q] += cbuf[q]
                pass_up(q).start()
            else:
                pass_up(2).wait_recv()

    def to_strip(w):
        return remote(
            nbuf.at[pl.ds(pl.multiple_of(w * STRIP, 8), STRIP + 16)], fbuf.at[1 + y],
            nsend.at[w], frecv.at[1 + y], w, me_t,
        )

    def to_side(w, plane, t):
        return remote(
            nbuf.at[pl.ds(pl.multiple_of(w * STRIP + 8, 8), STRIP)], fbuf.at[plane, pl.ds(8, STRIP)],
            hsend.at[w], frecv.at[plane], w, t,
        )

    to_later = jnp.logical_and(y == NY - 1, me_t < last)
    to_earlier = jnp.logical_and(y == 0, me_t > 0)

    @pl.when(c == 1)
    def _():
        nbuf[pl.ds(0, 8)] = jnp.zeros((8, Y), F32)
        nbuf[pl.ds(X + 8, 8)] = jnp.zeros((8, Y), F32)
        for p in range(4):
            for copy in last_down(p):
                copy.wait_recv()
            part = pl.ds(64 * p, 64)
            image = obuf[3, 0, part] + cbuf[3, 0, part] + cbuf[4, 0, part]
            light = obuf[3, 1, part] + cbuf[3, 1, part] + cbuf[4, 1, part]
            nbuf[pl.ds(64 * p + 8, 64)] = image / (1.0 + light)

            @pl.loop(2 * p, 2 * p + 2)
            def _(w):
                @pl.when(to_later)
                def _():
                    to_side(w, 0, me_t + 1).start()

                @pl.when(to_earlier)
                def _():
                    to_side(w, 5, me_t - 1).start()

            @pl.loop((0, 1, 3, 5)[p], (1, 3, 5, 8)[p])
            def _(w):
                @pl.when(w != me_w)
                def _():
                    to_strip(w).start()

        fbuf[1 + y] = nbuf[pl.ds(pl.multiple_of(me_w * STRIP, 8), STRIP + 16)]

    @pl.when(me_t == 0)
    def _():
        fbuf[0] = jnp.zeros((STRIP + 16, Y), F32)

    @pl.when(me_t == last)
    def _():
        fbuf[5] = jnp.zeros((STRIP + 16, Y), F32)

    for j in range(PLANES):

        @pl.when(jnp.logical_not(jnp.logical_and(c == 1, y == j)))
        def _():
            pltpu.make_async_copy(fbuf.at[1 + j], fbuf.at[1 + j], frecv.at[1 + j]).wait()

    @pl.when(me_t > 0)
    def _():
        pltpu.make_async_copy(fbuf.at[0, pl.ds(8, STRIP)], fbuf.at[0, pl.ds(8, STRIP)], frecv.at[0]).wait()

    @pl.when(me_t < last)
    def _():
        pltpu.make_async_copy(fbuf.at[5, pl.ds(8, STRIP)], fbuf.at[5, pl.ds(8, STRIP)], frecv.at[5]).wait()

    column = lax.broadcasted_iota(jnp.int32, (STRIP, Y), 1)
    for j in range(PLANES):
        center = fbuf[1 + j, pl.ds(8, STRIP)]
        beside = fbuf[j, pl.ds(8, STRIP)] + fbuf[2 + j, pl.ds(8, STRIP)]
        beside = beside + fbuf[1 + j, pl.ds(7, STRIP)] + fbuf[1 + j, pl.ds(9, STRIP)]
        before = jnp.where(column == 0, 0.0, pltpu.roll(center, 1, 1))
        after = jnp.where(column == Y - 1, 0.0, pltpu.roll(center, Y - 1, 1))
        out_ref[j] = beside + (before + after) - 6.0 * center

    for part, sem in ((head_out.at[pl.ds(0, 31), pl.ds(0, 136)], headsend), (sbuf.at[pl.ds(0, 93)], asend)):
        pltpu.make_async_copy(part, part, sem).wait()

    @pl.when(c == 0)
    def _():
        begin_up().wait_send()
        begin_down().wait_send()
        for q in range(1, 3):
            pass_down(q).wait_send()
        for p in range(4):
            for copy in last_down(p):
                copy.wait_send()

    @pl.when(c == 1)
    def _():
        for q in range(3):
            pass_up(q).wait_send()
        @pl.loop(1, NY * NC)
        def _(k):
            to_strip(lax.rem(me_w + k, NY * NC)).wait_send()

        @pl.loop(0, NY * NC)
        def _(w):
            @pl.when(to_later)
            def _():
                to_side(w, 0, me_t + 1).wait_send()

            @pl.when(to_earlier)
            def _():
                to_side(w, 5, me_t - 1).wait_send()


def per_device(source, receiver, corners):
    source = source.reshape(2, NX, NZ, PLANES, BX, BY)
    receiver = receiver.reshape(2, NX, NZ, PLANES, BX, BY)
    dma = pltpu.SemaphoreType.DMA
    return pl.pallas_call(
        kernel,
        out_shape=jax.ShapeDtypeStruct((PLANES, STRIP, Y), F32),
        in_specs=[
            pl.BlockSpec(memory_space=pltpu.HBM),
            pl.BlockSpec(memory_space=pltpu.HBM),
            pl.BlockSpec(memory_space=pltpu.HBM),
        ],
        out_specs=pl.BlockSpec(memory_space=pltpu.VMEM),
        scratch_shapes=[
            pltpu.SMEM((2, 2), jnp.int32),
            pltpu.VMEM((NZ, 2, 2, NX, NY, BX, BY), BF16),
            pltpu.VMEM((2 * NX * NY, 144, BY), BF16),
            pltpu.VMEM((6 * NX * NY, 128, BY), BF16),
            pltpu.VMEM((GROUP, 144, BY), BF16),
            pltpu.VMEM((3, GROUP, 128, BY), BF16),
            pltpu.VMEM((BLOCKS, X, 256), BF16),
            pltpu.VMEM((BLOCKS, 256, 128), BF16),
            pltpu.VMEM((4, 2, X, Y), F32),
            pltpu.VMEM((5, 2, X, Y), F32),
            pltpu.VMEM((X + 16, Y), F32),
            pltpu.VMEM((PLANES + 2, STRIP + 16, Y), F32),
            dma, dma((NZ, 2)), dma, dma, dma((4, BLOCKS)),
            dma((12,)), dma((12,)), dma((8,)), dma((8,)), dma((6,)),
        ],
        compiler_params=pltpu.CompilerParams(
            collective_id=0, has_side_effects=True, vmem_limit_bytes=56_000_000
        ),
        name="stack_shots",
    )(corners, source, receiver)


def solution(mesh):
    return jax.shard_map(
        per_device,
        mesh=mesh,
        in_specs=(
            P(("shot", "tile"), None, None, None, None),
            P(("shot", "tile"), None, None, None, None),
            P(("shot", "tile"), None),
        ),
        out_specs=P("tile", "shot", None),
        check_vma=False,
    )
```
